128 devices in a mesh: gx: 8 (over y, core), gy: 16 (over z, x).
Axes of the slice: x: 4, y: 4, z: 4, core: 2. Of those that a mesh axis runs over, the one named last changes fastest.
Arguments:
- transfer: bfloat16 [2048, 75, 128], P(('gx', 'gy')), may hold values from -6 to 6
- positions: float32 [2048, 3, 128], P(('gx', 'gy')), may hold values from -4 to 4
- normals: float32 [2048, 3, 128], P(('gx', 'gy')), may hold values from -4 to 4
- area: float32 [2048, 128], P(('gx', 'gy')), may hold values from 0.06 to 3
- albedo: float32 [2048, 3, 128], P(('gx', 'gy')), may hold values from 0.3 to 0.9
- pairs: int32 [2048, 40], P(('gx', 'gy')), may hold values from 0 to 2047, as said below
- home: int32 [2048], replicated, may hold values from 0 to 2047, as said below
Outputs:
- bounce_one: bfloat16 [2048, 75, 128], P(('gx', 'gy'))
- bounce_two: bfloat16 [2048, 75, 128], P(('gx', 'gy'))
- energies: float32 [2], replicated
The draws below stay inside these ranges and needn't reach their ends.
Inputs may be any that keep to these rules, and one draw needn't show every extreme that they name: `home`: A permutation; the block in slot s is held by device s // 16, devices counted gx major. `pairs`: the first 16 entries of a row name blocks held by the same device as the row's slot, the other 24 name blocks held by other devices. Over the rows of one device, the far entries name at most 2 distinct blocks of any one other device, and exactly 2 of some. Ids may repeat within a row; each entry counts.
All inputs are finite; a program needn't handle non-finite values.
Results may differ from the reference program's by a relative error of at most 0.02.
Values may be sent and summed in bfloat16 or wider, within the bound.
No kernel may reach another device: no remote copies, remote signals or barrier semaphores. Data moves between devices by JAX's collectives and lax.ppermute only.
A program may use at most 128 MiB of HBM per device.

```python
import jax
import jax.numpy as jnp
from jax import lax

BLK_DEV = 16
VERT = 128
COLORS = 3
NEAR = 16
FAR = 24
CAP = 2
CH = 75
BLOCKS = 2048


def layout_tables(key):
    devices_all = BLOCKS // BLK_DEV
    home = jax.random.permutation(jax.random.fold_in(key, 11), BLOCKS).astype(jnp.int32)
    inverse = jnp.argsort(home, stable=True).astype(jnp.int32)
    keys = jax.random.split(jax.random.fold_in(key, 12), 4)
    slot_all = jnp.arange(BLOCKS, dtype=jnp.int32)
    device_of = slot_all // BLK_DEV
    near_local = jax.random.randint(keys[0], (BLOCKS, NEAR), 0, BLK_DEV, dtype=jnp.int32)
    near_slot = device_of[:, None] * BLK_DEV + near_local
    offset = jax.random.randint(keys[1], (BLOCKS, FAR), 1, devices_all, dtype=jnp.int32)
    column = jnp.arange(FAR, dtype=jnp.int32)[None, :]
    forced = (slot_all % BLK_DEV == 0)[:, None] & (column < CAP)
    offset = jnp.where(forced, 1, offset)
    pick_k = jax.random.randint(keys[2], (BLOCKS, FAR), 0, CAP, dtype=jnp.int32)
    pick_k = jnp.where(forced, column, pick_k)
    owner_dev = (device_of[:, None] + offset) % devices_all
    start_tab = jax.random.randint(keys[3], (devices_all, devices_all), 0, BLK_DEV, dtype=jnp.int32)
    local_idx = (start_tab[device_of[:, None], owner_dev] + pick_k) % BLK_DEV
    far_slot = owner_dev * BLK_DEV + local_idx
    source_slot = jnp.concatenate([near_slot, far_slot], axis=1)
    pairs = jnp.take(inverse, source_slot, axis=0).astype(jnp.int32)
    return (home, pairs)


def draw_home(key, part):
    return layout_tables(key)[0]


def draw_pairs(key, part):
    return layout_tables(key)[1]


def draw_area(key, part):
    ramp = jnp.arange(BLOCKS, dtype=jnp.float32)[:, None] / (BLOCKS - 1)
    logs = jax.random.uniform(key, (BLOCKS, VERT), jnp.float32, jnp.log(0.2), jnp.log(2.0))
    return jnp.exp(logs) * (0.5 + ramp)


def shard_levels(own_key, extent, cuts, least, largest):
    gain, own = 1.0, jax.random.fold_in(own_key, 6)
    for position, blocks in cuts:
        draws = jnp.exp(jax.random.uniform(jax.random.fold_in(own, position), (blocks,), jnp.float32, least / len(cuts), largest / len(cuts)))
        gain = gain * jnp.repeat(draws, extent[position] // blocks).reshape([-1 if axis == position else 1 for axis in range(len(extent))])
    return gain


def bell_draw(stream_key, extent, spread, bound, cuts=(), kind=jnp.bfloat16):
    values = spread * jax.random.normal(stream_key, extent, jnp.float32)
    if cuts:
        values = values * shard_levels(stream_key, extent, cuts, -0.22, 0.18)
    return jnp.clip(values, -bound, bound).astype(kind)


def setup_inputs(seed: int = 0) -> dict:
    key_list = jax.random.split(jax.random.key(seed), 8)
    return {
        "transfer": bell_draw(key_list[0], (BLOCKS, CH, VERT), 1.0, 6.0, ((0, 128),)),
        "positions": bell_draw(key_list[1], (BLOCKS, 3, VERT), 1.0, 4.0, ((0, 128),), jnp.float32),
        "normals": bell_draw(key_list[2], (BLOCKS, 3, VERT), 1.0, 4.0, ((0, 128),), jnp.float32),
        "area": draw_area(jax.random.fold_in(key_list[7], 71), 0),
        "albedo": jnp.clip(0.3 + 0.59999996 * jax.random.uniform(key_list[4], (BLOCKS, COLORS, VERT), jnp.float32) ** shard_levels(key_list[4], (BLOCKS, COLORS, VERT), ((0, 128),), -0.2, 0.2), 0.3, 0.9),
        "pairs": draw_pairs(jax.random.fold_in(key_list[7], 71), 0),
        "home": draw_home(jax.random.fold_in(key_list[7], 71), 0),
    }


batch_blocks = 4


def form_tiles(recv_pos, recv_nrm, src_pos, src_nrm, src_area):
    distance = None
    along_p = None
    along_q = None
    for axis_id in range(3):
        gap_vec = src_pos[:, :, axis_id, None, :] - recv_pos[:, None, axis_id, :, None]
        near_term = recv_nrm[:, None, axis_id, :, None] * gap_vec
        far_term = src_nrm[:, :, axis_id, None, :] * gap_vec
        if distance is None:
            distance = gap_vec * gap_vec
            along_p = near_term
            along_q = far_term
        else:
            distance = distance + gap_vec * gap_vec
            along_p = along_p + near_term
            along_q = along_q + far_term
    soft_sq = distance + 1.0
    transfer_factors = jnp.maximum(along_p, 0.0) * jnp.maximum(-along_q, 0.0) * src_area[:, :, None, :] / (jnp.pi * soft_sq * soft_sq)
    return transfer_factors.astype(jnp.bfloat16)


def reflect_all(source_rows, src_positions, src_normals, src_area, pair_row_list, recv_positions, recv_normals):
    turns = pair_row_list.shape[0] // batch_blocks

    def group_term(group_id):
        first_row = group_id * batch_blocks
        picked_rows = lax.dynamic_slice_in_dim(pair_row_list, first_row, batch_blocks, 0)
        recv_pos = lax.dynamic_slice_in_dim(recv_positions, first_row, batch_blocks, 0)
        recv_nrm = lax.dynamic_slice_in_dim(recv_normals, first_row, batch_blocks, 0)
        transfer_factors = form_tiles(recv_pos, recv_nrm, jnp.take(src_positions, picked_rows, axis=0),
                             jnp.take(src_normals, picked_rows, axis=0), jnp.take(src_area, picked_rows, axis=0))
        collected_values = jnp.take(source_rows, picked_rows, axis=0)
        return jnp.einsum('wxmy,wxsy->wms', collected_values.astype(jnp.float32), transfer_factors.astype(jnp.float32))

    summed = lax.map(group_term, jnp.arange(turns, dtype=jnp.int32))
    return summed.reshape((pair_row_list.shape[0],) + source_rows.shape[1:])


def apply_albedo(summed, albedo):
    blocks_here, channels, verts = summed.shape
    shaped = summed.reshape(blocks_here, COLORS, channels // COLORS, verts) * albedo[:, :, None, :]
    return shaped.reshape(blocks_here, channels, verts)


def reference(transfer, positions, normals, area, albedo, pairs, home):
    slot_ids = jnp.take(home, pairs, axis=0)
    first_bounce = apply_albedo(reflect_all(transfer, positions, normals, area, slot_ids, positions, normals), albedo)
    bounce_one = first_bounce.astype(jnp.bfloat16)
    second_bounce = apply_albedo(reflect_all(bounce_one, positions, normals, area, slot_ids, positions, normals), albedo)
    bounce_two = second_bounce.astype(jnp.bfloat16)
    inv_count = 1.0 / (BLOCKS * VERT * CH)
    energy_one = jnp.sum(area[:, None, :] * first_bounce * first_bounce) * inv_count
    energy_two = jnp.sum(area[:, None, :] * second_bounce * second_bounce) * inv_count
    energies = jnp.stack([energy_one, energy_two]).astype(jnp.float32)
    return bounce_one, bounce_two, energies
```

```python
import functools
import math

import jax
import jax.numpy as jnp
from jax import lax
from jax.experimental import pallas as pl
from jax.experimental.pallas import tpu as pltpu
from jax.sharding import Mesh
from jax.sharding import PartitionSpec as P

COLORS = 3
NEAR = 16
FAR = 24
PAIRS = NEAR + FAR
CAP = 2
CH = 75
CHP = 80
BLK = 16
VERT = 128
DEVS = 128
ROWS = DEVS * CAP
AXES = ("gx_0", "gx_1", "gy_0", "gy_1")
CHUNK = 32

F32 = jnp.float32
BF16 = jnp.bfloat16
I32 = jnp.int32


def params(limit_mib=24):
    return pltpu.CompilerParams(
        dimension_semantics=("arbitrary",), vmem_limit_bytes=limit_mib * 1024 * 1024
    )


def cost(flops, read=0):
    return pl.CostEstimate(flops=int(flops), bytes_accessed=int(read), transcendentals=0)


def index_kernel(pairs_ref, home_ref, idx_ref, req_ref):
    home = home_ref[...]
    both = jnp.concatenate([home >> 4, home & 15], axis=0).astype(F32).astype(BF16)
    pairs = pairs_ref[...]
    low = pairs & 127
    high = pairs >> 7
    sub = lax.broadcasted_iota(I32, (VERT, PAIRS), 0)
    sub_f = sub.astype(F32)
    sub16 = lax.broadcasted_iota(I32, (16, PAIRS), 0)
    lane = lax.broadcasted_iota(I32, (VERT, PAIRS), 1)
    lane_row = lax.broadcasted_iota(I32, (1, PAIRS), 1)
    is_far = lane >= NEAR
    owners, locals_ = [], []
    least = jnp.full((VERT, PAIRS), 99.0, F32)
    most = jnp.full((VERT, PAIRS), -1.0, F32)
    for s in range(BLK):
        hot = jnp.where(sub == low[s : s + 1, :], 1.0, 0.0).astype(BF16)
        got = jnp.dot(both, hot, preferred_element_type=F32)
        here = sub16 == high[s : s + 1, :]
        owner = jnp.sum(jnp.where(here, got[:16], 0.0), axis=0, keepdims=True)
        local = jnp.sum(jnp.where(here, got[16:], 0.0), axis=0, keepdims=True)
        owners.append(owner)
        locals_.append(local)
        same = (sub_f == owner) & is_far
        least = jnp.minimum(least, jnp.where(same, local, 99.0))
        most = jnp.maximum(most, jnp.where(same, local, -1.0))
    lo = jnp.min(least, axis=1, keepdims=True)
    hi = jnp.max(most, axis=1, keepdims=True)
    for s in range(BLK):
        first = jnp.sum(jnp.where(sub_f == owners[s], lo, 0.0), axis=0, keepdims=True)
        far_row = owners[s] * 2.0 + jnp.where(locals_[s] == first, 0.0, 1.0)
        idx_ref[s : s + 1, :] = jnp.where(lane_row < NEAR, locals_[s], far_row).astype(I32)
    used = hi >= 0.0
    req_ref[:, 0:1] = jnp.where(used, lo, 0.0).astype(I32)
    req_ref[:, 1:2] = jnp.where(used, hi, 0.0).astype(I32)


def find_indices(pairs, home):
    return pl.pallas_call(
        index_kernel,
        out_shape=(
            jax.ShapeDtypeStruct((BLK, PAIRS), I32),
            jax.ShapeDtypeStruct((DEVS, CAP), I32),
        ),
        cost_estimate=cost(4e6),
        compiler_params=pltpu.CompilerParams(vmem_limit_bytes=8 * 1024 * 1024),
        name="indices",
    )(pairs, home.reshape(BLK, VERT))


def geometry_kernel(req_ref, pos_ref, nrm_ref, area_ref, out_ref, table):
    table[:, 0:3, :] = pos_ref[...]
    table[:, 3:6, :] = nrm_ref[...]
    table[:, 6:7, :] = area_ref[...]
    table[:, 7:8, :] = jnp.zeros((BLK, 1, VERT), F32)

    def put(i, carry):
        out_ref[i] = table[req_ref[i]].astype(BF16)
        return carry

    lax.fori_loop(0, ROWS, put, 0, unroll=8)


def pack_geometry(req, pos, nrm, area):
    whole = lambda *shape: pl.BlockSpec(shape, lambda i, *_: (0,) * len(shape))
    return pl.pallas_call(
        geometry_kernel,
        grid_spec=pltpu.PrefetchScalarGridSpec(
            num_scalar_prefetch=1,
            grid=(1,),
            in_specs=[whole(BLK, 3, VERT), whole(BLK, 3, VERT), whole(BLK, 1, VERT)],
            out_specs=whole(ROWS, 8, VERT),
            scratch_shapes=[pltpu.VMEM((BLK, 8, VERT), F32)],
        ),
        out_shape=jax.ShapeDtypeStruct((ROWS, 8, VERT), BF16),
        cost_estimate=cost(2e6),
        compiler_params=params(8),
        name="pack_geometry",
    )(req, pos, nrm, area)


def send_kernel(req_ref, field_ref, out_ref, slab, sem):
    slab[:, 64:, :] = jnp.zeros((BLK, CHP - 64, VERT), BF16)
    slab[:, :CH, :] = field_ref[...]

    def put(i, carry):
        pltpu.make_async_copy(slab.at[req_ref[i]], out_ref.at[i], sem).start()
        return carry

    lax.fori_loop(0, ROWS, put, 0, unroll=8)
    pltpu.make_async_copy(out_ref, out_ref, sem).wait()


def pack_field(req, field):
    return pl.pallas_call(
        send_kernel,
        grid_spec=pltpu.PrefetchScalarGridSpec(
            num_scalar_prefetch=1,
            grid=(1,),
            in_specs=[pl.BlockSpec((BLK, CH, VERT), lambda i, *_: (0, 0, 0))],
            out_specs=pl.BlockSpec(memory_space=pl.ANY),
            scratch_shapes=[pltpu.VMEM((BLK, CHP, VERT), BF16), pltpu.SemaphoreType.DMA],
        ),
        out_shape=jax.ShapeDtypeStruct((ROWS, CHP, VERT), BF16),
        cost_estimate=cost(1e7),
        compiler_params=params(8),
        name="pack_field",
    )(req, field)


def fill_tiles(index_of, count, slot_geo, table, out_ref):
    columns = slot_geo.T
    for c in range(VERT // CHUNK):
        part = columns[c * CHUNK : (c + 1) * CHUNK]
        recv = [jnp.broadcast_to(part[:, i : i + 1], (CHUNK, VERT)) for i in range(6)]

        def one(j, carry, c=c, recv=recv):
            rows = table[index_of(j)]
            gap = [rows[i : i + 1] - recv[i] for i in range(3)]
            soft = gap[0] * gap[0] + gap[1] * gap[1] + gap[2] * gap[2] + 1.0
            near = recv[3] * gap[0] + recv[4] * gap[1] + recv[5] * gap[2]
            far = rows[3:4] * gap[0] + rows[4:5] * gap[1] + rows[5:6] * gap[2]
            value = jnp.maximum(near, 0.0) * jnp.maximum(far, 0.0) / (soft * soft)
            at = pl.multiple_of(j * VERT, VERT)
            out_ref[0, c * CHUNK : (c + 1) * CHUNK, pl.ds(at, VERT)] = value.astype(BF16)
            return carry

        lax.fori_loop(0, count, one, 0, unroll=4)


def scaled(normal, area):
    return normal * (area * (-1.0 / math.pi))


def product(left, right):
    return lax.dot_general(left, right, (((1,), (1,)), ((), ())), preferred_element_type=F32)


def near_kernel(idx_ref, field_ref, pos_ref, nrm_ref, area_ref, tiles_ref, sum_ref, table, geo, rows):
    s = pl.program_id(0)

    @pl.when(s == 0)
    def _():
        table[:, 0:3, :] = pos_ref[...]
        table[:, 3:6, :] = scaled(nrm_ref[...], area_ref[...])
        table[:, 6:8, :] = jnp.zeros((BLK, 2, VERT), F32)
        geo[:, 0:3, :] = pos_ref[...]
        geo[:, 3:6, :] = nrm_ref[...]
        geo[:, 6:8, :] = jnp.zeros((BLK, 2, VERT), F32)

    fill_tiles(lambda j: idx_ref[s * PAIRS + j], NEAR, geo[s], table, tiles_ref)
    for j in range(NEAR):
        rows[:, j * VERT : (j + 1) * VERT] = field_ref[idx_ref[s * PAIRS + j]]
    sum_ref[0] = product(rows[...], tiles_ref[0])


def near_first(idx, field, pos, nrm, area):
    whole = lambda *shape: pl.BlockSpec(shape, lambda i, *_: (0,) * len(shape))
    return pl.pallas_call(
        near_kernel,
        grid_spec=pltpu.PrefetchScalarGridSpec(
            num_scalar_prefetch=1,
            grid=(BLK,),
            in_specs=[
                whole(BLK, CH, VERT),
                whole(BLK, 3, VERT),
                whole(BLK, 3, VERT),
                whole(BLK, 1, VERT),
            ],
            out_specs=[
                pl.BlockSpec((1, VERT, NEAR * VERT), lambda i, *_: (i, 0, 0)),
                pl.BlockSpec((1, CH, VERT), lambda i, *_: (i, 0, 0)),
            ],
            scratch_shapes=[
                pltpu.VMEM((BLK, 8, VERT), F32),
                pltpu.VMEM((BLK, 8, VERT), F32),
                pltpu.VMEM((CH, NEAR * VERT), BF16),
            ],
        ),
        out_shape=(
            jax.ShapeDtypeStruct((BLK, VERT, NEAR * VERT), BF16),
            jax.ShapeDtypeStruct((BLK, CH, VERT), F32),
        ),
        cost_estimate=cost(6e8),
        compiler_params=params(),
        name="near_first",
    )(idx, field, pos, nrm, area)


def near_again_kernel(idx_ref, field_ref, tiles_ref, sum_ref, rows):
    s = pl.program_id(0)
    for j in range(NEAR):
        rows[:, j * VERT : (j + 1) * VERT] = field_ref[idx_ref[s * PAIRS + j]]
    sum_ref[0] = product(rows[...], tiles_ref[0])


def near_again(idx, field, tiles):
    return pl.pallas_call(
        near_again_kernel,
        grid_spec=pltpu.PrefetchScalarGridSpec(
            num_scalar_prefetch=1,
            grid=(BLK,),
            in_specs=[
                pl.BlockSpec((BLK, CH, VERT), lambda i, *_: (0, 0, 0)),
                pl.BlockSpec((1, VERT, NEAR * VERT), lambda i, *_: (i, 0, 0)),
            ],
            out_specs=pl.BlockSpec((1, CH, VERT), lambda i, *_: (i, 0, 0)),
            scratch_shapes=[pltpu.VMEM((CH, NEAR * VERT), BF16)],
        ),
        out_shape=jax.ShapeDtypeStruct((BLK, CH, VERT), F32),
        cost_estimate=cost(3e8),
        compiler_params=params(),
        name="near_again",
    )(idx, field, tiles)


def far_tiles_kernel(idx_ref, got_ref, pos_ref, nrm_ref, tiles_ref, table, geo):
    s = pl.program_id(0)

    @pl.when(s == 0)
    def _():
        got = got_ref[...].astype(F32)
        table[:, 0:3, :] = got[:, 0:3]
        table[:, 3:6, :] = scaled(got[:, 3:6], got[:, 6:7])
        table[:, 6:8, :] = jnp.zeros((ROWS, 2, VERT), F32)
        geo[:, 0:3, :] = pos_ref[...]
        geo[:, 3:6, :] = nrm_ref[...]
        geo[:, 6:8, :] = jnp.zeros((BLK, 2, VERT), F32)

    fill_tiles(lambda j: idx_ref[s * PAIRS + NEAR + j], FAR, geo[s], table, tiles_ref)


def far_tiles(idx, got, pos, nrm):
    whole = lambda *shape: pl.BlockSpec(shape, lambda i, *_: (0,) * len(shape))
    return pl.pallas_call(
        far_tiles_kernel,
        grid_spec=pltpu.PrefetchScalarGridSpec(
            num_scalar_prefetch=1,
            grid=(BLK,),
            in_specs=[whole(ROWS, 8, VERT), whole(BLK, 3, VERT), whole(BLK, 3, VERT)],
            out_specs=pl.BlockSpec((1, VERT, FAR * VERT), lambda i, *_: (i, 0, 0)),
            scratch_shapes=[pltpu.VMEM((ROWS, 8, VERT), F32), pltpu.VMEM((BLK, 8, VERT), F32)],
        ),
        out_shape=jax.ShapeDtypeStruct((BLK, VERT, FAR * VERT), BF16),
        cost_estimate=cost(6e8),
        compiler_params=params(),
        name="far_tiles",
    )(idx, got, pos, nrm)


def far_kernel(idx_ref, got_ref, tiles_ref, near_ref, albedo_ref, area_ref, out_ref, energy_ref, rows):
    s = pl.program_id(0)
    for j in range(FAR):
        rows[:, j * VERT : (j + 1) * VERT] = got_ref[idx_ref[s * PAIRS + NEAR + j]]
    total = near_ref[0] + product(rows[...], tiles_ref[0])[:CH]
    channel = lax.broadcasted_iota(I32, (CH, VERT), 0)
    shade = jnp.where(
        channel < CH // COLORS,
        albedo_ref[0, 0:1, :],
        jnp.where(channel < 2 * (CH // COLORS), albedo_ref[0, 1:2, :], albedo_ref[0, 2:3, :]),
    )
    bounce = total * shade
    out_ref[0] = bounce.astype(BF16)
    share = jnp.sum(area_ref[0] * bounce * bounce, axis=0, keepdims=True)

    @pl.when(s == 0)
    def _():
        energy_ref[...] = share

    @pl.when(s > 0)
    def _():
        energy_ref[...] = energy_ref[...] + share


def far_bounce(idx, got, tiles, near, albedo, area):
    slot = lambda *shape: pl.BlockSpec((1,) + shape, lambda i, *_: (i, 0, 0))
    return pl.pallas_call(
        far_kernel,
        grid_spec=pltpu.PrefetchScalarGridSpec(
            num_scalar_prefetch=1,
            grid=(BLK,),
            in_specs=[
                pl.BlockSpec((ROWS, CHP, VERT), lambda i, *_: (0, 0, 0)),
                slot(VERT, FAR * VERT),
                slot(CH, VERT),
                slot(COLORS, VERT),
                slot(1, VERT),
            ],
            out_specs=[slot(CH, VERT), pl.BlockSpec((1, VERT), lambda i, *_: (0, 0))],
            scratch_shapes=[pltpu.VMEM((CHP, FAR * VERT), BF16)],
        ),
        out_shape=(
            jax.ShapeDtypeStruct((BLK, CH, VERT), BF16),
            jax.ShapeDtypeStruct((1, VERT), F32),
        ),
        cost_estimate=cost(5e8),
        compiler_params=params(),
        name="far_bounce",
    )(idx, got, tiles, near, albedo, area)


def swap(value):
    return lax.all_to_all(value, AXES, split_axis=0, concat_axis=0, tiled=True)


def body(transfer, positions, normals, area, albedo, pairs, home):
    area_row = area.reshape(BLK, 1, VERT)
    idx, need = find_indices(pairs, home)
    idx = idx.reshape(-1)
    asked = swap(need).reshape(-1)
    near_tiles, near_one = near_first(idx, transfer, positions, normals, area_row)
    geometry = swap(pack_geometry(asked, positions, normals, area_row))
    got_one = swap(pack_field(asked, transfer))
    tiles = far_tiles(idx, geometry, positions, normals)
    bounce_one, share_one = far_bounce(idx, got_one, tiles, near_one, albedo, area_row)
    got_two = swap(pack_field(asked, bounce_one))
    near_two = near_again(idx, bounce_one, near_tiles)
    bounce_two, share_two = far_bounce(idx, got_two, tiles, near_two, albedo, area_row)
    shares = jnp.concatenate([share_one, share_two], axis=0)
    shares = swap(jnp.broadcast_to(shares[None], (DEVS, 2, VERT)))
    energies = jnp.sum(shares, axis=(0, 2)) * (1.0 / (DEVS * BLK * VERT * CH))
    return bounce_one, bounce_two, energies


def solution(mesh):
    finer = Mesh(mesh.devices.reshape(4, 2, 4, 4), AXES)
    three = P(AXES, None, None)
    return jax.shard_map(
        body,
        mesh=finer,
        in_specs=(three, three, three, P(AXES, None), three, P(AXES, None), P()),
        out_specs=(three, three, P()),
        check_vma=False,
    )
```

```python
import functools
import math

import jax
import jax.numpy as jnp
from jax import lax
from jax.experimental import pallas as pl
from jax.experimental.pallas import tpu as pltpu
from jax.sharding import Mesh
from jax.sharding import PartitionSpec as P

COLORS = 3
NEAR = 16
FAR = 24
PAIRS = NEAR + FAR
CAP = 2
CH = 75
CHP = 80
BLK = 16
VERT = 128
DEVS = 128
ROWS = DEVS * CAP
AXES = ("gx_0", "gx_1", "gy_0", "gy_1")

F32 = jnp.float32
BF16 = jnp.bfloat16
I32 = jnp.int32


def params(limit_mib=40):
    return pltpu.CompilerParams(
        dimension_semantics=("arbitrary",), vmem_limit_bytes=limit_mib * 1024 * 1024
    )


def cost(flops, read=0):
    return pl.CostEstimate(flops=int(flops), bytes_accessed=int(read), transcendentals=0)


def index_kernel(pairs_ref, home_ref, idx_ref, req_ref):
    home = home_ref[...]
    both = jnp.concatenate([home >> 4, home & 15], axis=0).astype(F32).astype(BF16)
    pairs = pairs_ref[...]
    low = pairs & 127
    high = pairs >> 7
    sub = lax.broadcasted_iota(I32, (VERT, PAIRS), 0)
    sub_f = sub.astype(F32)
    sub16 = lax.broadcasted_iota(I32, (16, PAIRS), 0)
    lane = lax.broadcasted_iota(I32, (VERT, PAIRS), 1)
    lane_row = lax.broadcasted_iota(I32, (1, PAIRS), 1)
    is_far = lane >= NEAR
    owners, locals_ = [], []
    least = jnp.full((VERT, PAIRS), 99.0, F32)
    most = jnp.full((VERT, PAIRS), -1.0, F32)
    for s in range(BLK):
        hot = jnp.where(sub == low[s : s + 1, :], 1.0, 0.0).astype(BF16)
        got = jnp.dot(both, hot, preferred_element_type=F32)
        here = sub16 == high[s : s + 1, :]
        owner = jnp.sum(jnp.where(here, got[:16], 0.0), axis=0, keepdims=True)
        local = jnp.sum(jnp.where(here, got[16:], 0.0), axis=0, keepdims=True)
        owners.append(owner)
        locals_.append(local)
        same = (sub_f == owner) & is_far
        least = jnp.minimum(least, jnp.where(same, local, 99.0))
        most = jnp.maximum(most, jnp.where(same, local, -1.0))
    lo = jnp.min(least, axis=1, keepdims=True)
    hi = jnp.max(most, axis=1, keepdims=True)
    for s in range(BLK):
        first = jnp.sum(jnp.where(sub_f == owners[s], lo, 0.0), axis=0, keepdims=True)
        far_row = owners[s] * 2.0 + jnp.where(locals_[s] == first, 0.0, 1.0)
        idx_ref[s : s + 1, :] = jnp.where(lane_row < NEAR, locals_[s], far_row).astype(I32)
    used = hi >= 0.0
    req_ref[:, 0:1] = jnp.where(used, lo, 0.0).astype(I32)
    req_ref[:, 1:2] = jnp.where(used, hi, 0.0).astype(I32)


def find_indices(pairs, home):
    return pl.pallas_call(
        index_kernel,
        out_shape=(
            jax.ShapeDtypeStruct((BLK, PAIRS), I32),
            jax.ShapeDtypeStruct((DEVS, CAP), I32),
        ),
        cost_estimate=cost(4e6),
        compiler_params=pltpu.CompilerParams(vmem_limit_bytes=8 * 1024 * 1024),
        name="indices",
    )(pairs, home.reshape(BLK, VERT))


def whole(*shape):
    return pl.BlockSpec(shape, lambda i, *_: (0,) * len(shape))


def slot(*shape):
    return pl.BlockSpec((1,) + shape, lambda i, *_: (i,) + (0,) * len(shape))


def in_hbm(value):
    return pltpu.with_memory_space_constraint(value, pltpu.HBM)


def grid_spec(prefetch, steps, in_specs, out_specs, scratch):
    return pltpu.PrefetchScalarGridSpec(
        num_scalar_prefetch=prefetch,
        grid=(steps,),
        in_specs=in_specs,
        out_specs=out_specs,
        scratch_shapes=scratch,
    )


def geometry_kernel(req_ref, pos_ref, nrm_ref, area_ref, out_ref, table):
    table[:, 0:3, :] = pos_ref[...]
    table[:, 3:6, :] = nrm_ref[...] * (area_ref[...] * (-1.0 / math.pi))
    table[:, 6:8, :] = jnp.ones((BLK, 2, VERT), F32)

    def put(i, carry):
        out_ref[i] = table[req_ref[i]].astype(BF16)
        return carry

    lax.fori_loop(0, ROWS, put, 0, unroll=8)


def pack_geometry(req, pos, nrm, area):
    return pl.pallas_call(
        geometry_kernel,
        grid_spec=grid_spec(
            1,
            1,
            [whole(BLK, 3, VERT), whole(BLK, 3, VERT), whole(BLK, 1, VERT)],
            whole(ROWS, 8, VERT),
            [pltpu.VMEM((BLK, 8, VERT), F32)],
        ),
        out_shape=jax.ShapeDtypeStruct((ROWS, 8, VERT), BF16),
        cost_estimate=cost(2e6),
        compiler_params=params(8),
        name="pack_geometry",
    )(req, pos, nrm, area)


PACK = 32


def send_kernel(req_ref, field_ref, out_ref, slab):
    step = pl.program_id(0)

    @pl.when(step == 0)
    def _():
        slab[:, 64:, :] = jnp.zeros((BLK, CHP - 64, VERT), BF16)
        slab[:, :CH, :] = field_ref[...]

    def put(i, carry):
        out_ref[i] = slab[req_ref[step * PACK + i]]
        return carry

    lax.fori_loop(0, PACK, put, 0, unroll=4)


def pack_field(req, field):
    return pl.pallas_call(
        send_kernel,
        grid_spec=grid_spec(
            1,
            ROWS // PACK,
            [whole(BLK, CH, VERT)],
            pl.BlockSpec((PACK, CHP, VERT), lambda i, *_: (i, 0, 0)),
            [pltpu.VMEM((BLK, CHP, VERT), BF16)],
        ),
        out_shape=pltpu.HBM((ROWS, CHP, VERT), BF16),
        cost_estimate=cost(1e7),
        compiler_params=params(8),
        name="pack_field",
    )(req, field)


def thirds(value):
    high = value.astype(BF16).astype(F32)
    rest = value - high
    middle = rest.astype(BF16).astype(F32)
    return high, middle, (rest - middle).astype(BF16).astype(F32)


NEAR_TERMS = ((0, 0), (0, 1), (1, 0), (1, 1), (0, 2), (2, 0))
FAR_TERMS = ((0, 0), (0, 1), (0, 2))


def stack_rows(parts):
    return jnp.concatenate(parts, axis=0)


def source_rows(geo, terms):
    parts = thirds(geo) if len(terms) > 3 else (geo,)
    square = geo[0:1] * geo[0:1] + geo[1:2] * geo[1:2] + geo[2:3] * geo[2:3] + 1.0
    facing = geo[3:4] * geo[0:1] + geo[4:5] * geo[1:2] + geo[5:6] * geo[2:3]
    zero = jnp.zeros((1, VERT), F32)
    alone = stack_rows([*thirds(square), *thirds(facing), zero, zero])
    return stack_rows([*[parts[i] for i, _ in terms], alone]).T.astype(BF16)


def receiver_rows(pos, nrm, terms):
    zero = jnp.zeros((1, VERT), F32)
    zeros3 = jnp.zeros((3, VERT), F32)
    one = jnp.ones((1, VERT), F32)
    square = pos[0:1] * pos[0:1] + pos[1:2] * pos[1:2] + pos[2:3] * pos[2:3]
    facing = nrm[0:1] * pos[0:1] + nrm[1:2] * pos[1:2] + nrm[2:3] * pos[2:3]
    forms = (
        (stack_rows([-2.0 * pos, zeros3, square, zero]), (1.0, 0.0)),
        (stack_rows([nrm, zeros3, -facing, zero]), (0.0, 0.0)),
        (stack_rows([zeros3, -pos, zero, zero]), (0.0, 1.0)),
    )
    out = []
    for rows, (with_square, with_facing) in forms:
        parts = thirds(rows)
        alone = stack_rows([one * with_square] * 3 + [one * with_facing] * 3 + [zero, zero])
        out.append(stack_rows([*[parts[j] for _, j in terms], alone]))
    return jnp.concatenate(out, axis=1).astype(BF16)


def fill_tiles(index_of, count, recv, table, out_ref):
    right = recv[...]
    for j in range(count):
        got = jnp.dot(table[index_of(j)], right, preferred_element_type=F32)
        soft = got[:, :VERT]
        value = jnp.maximum(got[:, VERT : 2 * VERT], 0.0) * jnp.maximum(got[:, 2 * VERT :], 0.0)
        value = value / (soft * soft)
        out_ref[0, j * VERT : (j + 1) * VERT, :] = value.astype(BF16)


def product(left, right):
    return jnp.dot(left, right, preferred_element_type=F32)


def near_kernel(idx_ref, field_ref, pos_ref, nrm_ref, area_ref, tiles_ref, sum_ref, table, recv, rows):
    s = pl.program_id(0)

    @pl.when(s == 0)
    def _():
        def make(t, carry):
            scaled = nrm_ref[t] * (area_ref[t] * (-1.0 / math.pi))
            geo = stack_rows([pos_ref[t], scaled, jnp.ones((2, VERT), F32)])
            table[t] = source_rows(geo, NEAR_TERMS)
            return carry

        lax.fori_loop(0, BLK, make, 0)

    recv[...] = receiver_rows(pos_ref[s], nrm_ref[s], NEAR_TERMS)
    fill_tiles(lambda j: idx_ref[s * PAIRS + j], NEAR, recv, table, tiles_ref)
    for j in range(NEAR):
        rows[:, j * VERT : (j + 1) * VERT] = field_ref[idx_ref[s * PAIRS + j]]
    sum_ref[0] = product(rows[...], tiles_ref[0])


NEAR_K = 8 * (len(NEAR_TERMS) + 1)
FAR_K = 8 * (len(FAR_TERMS) + 1)


def near_first(idx, field, pos, nrm, area):
    return pl.pallas_call(
        near_kernel,
        grid_spec=grid_spec(
            1,
            BLK,
            [whole(BLK, CH, VERT), whole(BLK, 3, VERT), whole(BLK, 3, VERT), whole(BLK, 1, VERT)],
            [slot(NEAR * VERT, VERT), slot(CH, VERT)],
            [
                pltpu.VMEM((BLK, VERT, NEAR_K), BF16),
                pltpu.VMEM((NEAR_K, 3 * VERT), BF16),
                pltpu.VMEM((CH, NEAR * VERT), BF16),
            ],
        ),
        out_shape=(
            pltpu.HBM((BLK, NEAR * VERT, VERT), BF16),
            jax.ShapeDtypeStruct((BLK, CH, VERT), F32),
        ),
        cost_estimate=cost(6e8),
        compiler_params=params(),
        name="near_first",
    )(idx, field, pos, nrm, area)


def near_again_kernel(idx_ref, field_ref, tiles_ref, sum_ref, rows, tiles, sems):
    s = pl.program_id(0)

    def copies(at):
        return pltpu.make_async_copy(tiles_ref.at[at], tiles.at[at], sems.at[at])

    @pl.when(s == 0)
    def _():
        for at in range(BLK):
            copies(at).start()

    copies(s).wait()
    for j in range(NEAR):
        rows[:, j * VERT : (j + 1) * VERT] = field_ref[idx_ref[s * PAIRS + j]]
    sum_ref[0] = product(rows[...], tiles[s])


def near_again(idx, field, tiles):
    return pl.pallas_call(
        near_again_kernel,
        grid_spec=grid_spec(
            1,
            BLK,
            [whole(BLK, CH, VERT), pl.BlockSpec(memory_space=pltpu.HBM)],
            slot(CH, VERT),
            [
                pltpu.VMEM((CH, NEAR * VERT), BF16),
                pltpu.VMEM((BLK, NEAR * VERT, VERT), BF16),
                pltpu.SemaphoreType.DMA((BLK,)),
            ],
        ),
        out_shape=jax.ShapeDtypeStruct((BLK, CH, VERT), F32),
        cost_estimate=cost(3e8),
        compiler_params=params(),
        name="near_again",
    )(idx, field, in_hbm(tiles))


def far_tiles_kernel(idx_ref, got_ref, pos_ref, nrm_ref, tiles_ref, table, recv):
    s = pl.program_id(0)

    @pl.when(s == 0)
    def _():
        def make(t, carry):
            table[t] = source_rows(got_ref[t].astype(F32), FAR_TERMS)
            return carry

        lax.fori_loop(0, ROWS, make, 0, unroll=4)

    recv[...] = receiver_rows(pos_ref[s], nrm_ref[s], FAR_TERMS)
    fill_tiles(lambda j: idx_ref[s * PAIRS + NEAR + j], FAR, recv, table, tiles_ref)


def far_tiles(idx, got, pos, nrm):
    return pl.pallas_call(
        far_tiles_kernel,
        grid_spec=grid_spec(
            1,
            BLK,
            [whole(ROWS, 8, VERT), whole(BLK, 3, VERT), whole(BLK, 3, VERT)],
            slot(FAR * VERT, VERT),
            [pltpu.VMEM((ROWS, VERT, FAR_K), BF16), pltpu.VMEM((FAR_K, 3 * VERT), BF16)],
        ),
        out_shape=pltpu.HBM((BLK, FAR * VERT, VERT), BF16),
        cost_estimate=cost(6e8),
        compiler_params=params(),
        name="far_tiles",
    )(idx, got, pos, nrm)


def far_kernel(
    idx_ref, got_ref, tiles_ref, near_ref, albedo_ref, area_ref, out_ref, energy_ref, rows, field, tiles, sems
):
    s = pl.program_id(0)

    def copies(at):
        return pltpu.make_async_copy(tiles_ref.at[at], tiles.at[at], sems.at[at])

    @pl.when(s == 0)
    def _():
        whole_field = pltpu.make_async_copy(got_ref, field, sems.at[BLK])
        whole_field.start()
        for at in range(BLK):
            copies(at).start()
        whole_field.wait()

    copies(s).wait()
    for j in range(FAR):
        rows[:, j * VERT : (j + 1) * VERT] = field[idx_ref[s * PAIRS + NEAR + j]]
    total = near_ref[0] + product(rows[...], tiles[s])[:CH]
    channel = lax.broadcasted_iota(I32, (CH, VERT), 0)
    shade = jnp.where(
        channel < CH // COLORS,
        albedo_ref[0, 0:1, :],
        jnp.where(channel < 2 * (CH // COLORS), albedo_ref[0, 1:2, :], albedo_ref[0, 2:3, :]),
    )
    bounce = total * shade
    out_ref[0] = bounce.astype(BF16)
    share = jnp.sum(area_ref[0] * bounce * bounce, axis=0, keepdims=True)

    @pl.when(s == 0)
    def _():
        energy_ref[...] = share

    @pl.when(s > 0)
    def _():
        energy_ref[...] = energy_ref[...] + share


def far_bounce(idx, got, tiles, near, albedo, area):
    return pl.pallas_call(
        far_kernel,
        grid_spec=grid_spec(
            1,
            BLK,
            [
                pl.BlockSpec(memory_space=pltpu.HBM),
                pl.BlockSpec(memory_space=pltpu.HBM),
                slot(CH, VERT),
                slot(COLORS, VERT),
                slot(1, VERT),
            ],
            [slot(CH, VERT), whole(1, VERT)],
            [
                pltpu.VMEM((CHP, FAR * VERT), BF16),
                pltpu.VMEM((ROWS, CHP, VERT), BF16),
                pltpu.VMEM((BLK, FAR * VERT, VERT), BF16),
                pltpu.SemaphoreType.DMA((BLK + 1,)),
            ],
        ),
        out_shape=(
            jax.ShapeDtypeStruct((BLK, CH, VERT), BF16),
            jax.ShapeDtypeStruct((1, VERT), F32),
        ),
        cost_estimate=cost(5e8),
        compiler_params=params(),
        name="far_bounce",
    )(idx, got, in_hbm(tiles), near, albedo, area)


def swap(value):
    return lax.all_to_all(value, AXES, split_axis=0, concat_axis=0, tiled=True)


def body(transfer, positions, normals, area, albedo, pairs, home):
    area_row = area.reshape(BLK, 1, VERT)
    idx, need = find_indices(pairs, home)
    idx = idx.reshape(-1)
    asked = swap(need).reshape(-1)
    near_tiles, near_one = near_first(idx, transfer, positions, normals, area_row)
    geometry = swap(pack_geometry(asked, positions, normals, area_row))
    got_one = swap(pack_field(asked, transfer))
    tiles = far_tiles(idx, geometry, positions, normals)
    bounce_one, share_one = far_bounce(idx, got_one, tiles, near_one, albedo, area_row)
    got_two = swap(pack_field(asked, bounce_one))
    near_two = near_again(idx, bounce_one, near_tiles)
    bounce_two, share_two = far_bounce(idx, got_two, tiles, near_two, albedo, area_row)
    shares = jnp.concatenate([share_one, share_two], axis=0)
    shares = swap(jnp.broadcast_to(shares[None], (DEVS, 2, VERT)))
    energies = jnp.sum(shares, axis=(0, 2)) * (1.0 / (DEVS * BLK * VERT * CH))
    return bounce_one, bounce_two, energies


def solution(mesh):
    finer = Mesh(mesh.devices.reshape(4, 2, 4, 4), AXES)
    three = P(AXES, None, None)
    return jax.shard_map(
        body,
        mesh=finer,
        in_specs=(three, three, three, P(AXES, None), three, P(AXES, None), P()),
        out_specs=(three, three, P()),
        check_vma=False,
    )
```

```python
import functools
import math

import jax
import jax.numpy as jnp
from jax import lax
from jax.experimental import pallas as pl
from jax.experimental.pallas import tpu as pltpu
from jax.sharding import Mesh
from jax.sharding import PartitionSpec as P

COLORS = 3
NEAR = 16
FAR = 24
PAIRS = NEAR + FAR
CAP = 2
CH = 75
MAIN = 64
REST = CH - MAIN
SECOND = 12
WIRE = 2 * MAIN + 24
BLK = 16
VERT = 128
DEVS = 128
ROWS = DEVS * CAP
AXES = ("gx_0", "gx_1", "gy_0", "gy_1")

F32 = jnp.float32
BF16 = jnp.bfloat16
I32 = jnp.int32


def in_hbm(value):
    return pltpu.with_memory_space_constraint(value, pltpu.HBM)


def params(limit_mib=40):
    return pltpu.CompilerParams(
        dimension_semantics=("arbitrary",), vmem_limit_bytes=limit_mib * 1024 * 1024
    )


def cost(flops, read=0):
    return pl.CostEstimate(flops=int(flops), bytes_accessed=int(read), transcendentals=0)


def index_kernel(pairs_hbm, home_hbm, idx_ref, req_ref, pairs_ref, home_ref, sems):
    first = pltpu.make_async_copy(pairs_hbm, pairs_ref, sems.at[0])
    second = pltpu.make_async_copy(home_hbm, home_ref, sems.at[1])
    first.start()
    second.start()
    first.wait()
    second.wait()
    home = home_ref[...]
    both = jnp.concatenate([home >> 4, home & 15], axis=0).astype(F32).astype(BF16)
    pairs = pairs_ref[...]
    low = pairs & 127
    high = pairs >> 7
    sub = lax.broadcasted_iota(I32, (VERT, PAIRS), 0)
    sub_f = sub.astype(F32)
    sub16 = lax.broadcasted_iota(I32, (16, PAIRS), 0)
    lane = lax.broadcasted_iota(I32, (VERT, PAIRS), 1)
    lane_row = lax.broadcasted_iota(I32, (1, PAIRS), 1)
    is_far = lane >= NEAR
    owners, locals_ = [], []
    least = jnp.full((VERT, PAIRS), 99.0, F32)
    most = jnp.full((VERT, PAIRS), -1.0, F32)
    for s in range(BLK):
        hot = jnp.where(sub == low[s : s + 1, :], 1.0, 0.0).astype(BF16)
        got = jnp.dot(both, hot, preferred_element_type=F32)
        here = sub16 == high[s : s + 1, :]
        owner = jnp.sum(jnp.where(here, got[:16], 0.0), axis=0, keepdims=True)
        local = jnp.sum(jnp.where(here, got[16:], 0.0), axis=0, keepdims=True)
        owners.append(owner)
        locals_.append(local)
        same = (sub_f == owner) & is_far
        least = jnp.minimum(least, jnp.where(same, local, 99.0))
        most = jnp.maximum(most, jnp.where(same, local, -1.0))
    lo = jnp.min(least, axis=1, keepdims=True)
    hi = jnp.max(most, axis=1, keepdims=True)
    for s in range(BLK):
        first = jnp.sum(jnp.where(sub_f == owners[s], lo, 0.0), axis=0, keepdims=True)
        far_row = owners[s] * 2.0 + jnp.where(locals_[s] == first, 0.0, 1.0)
        idx_ref[s : s + 1, :] = jnp.where(lane_row < NEAR, locals_[s], far_row).astype(I32)
    used = hi >= 0.0
    req_ref[:, 0:1] = jnp.where(used, lo, 0.0).astype(I32)
    req_ref[:, 1:2] = jnp.where(used, hi, 0.0).astype(I32)


def find_indices(pairs, home):
    return pl.pallas_call(
        index_kernel,
        out_shape=(
            jax.ShapeDtypeStruct((BLK, PAIRS), I32),
            jax.ShapeDtypeStruct((DEVS, CAP), I32),
        ),
        in_specs=[pl.BlockSpec(memory_space=pltpu.HBM), pl.BlockSpec(memory_space=pltpu.HBM)],
        scratch_shapes=[
            pltpu.VMEM((BLK, PAIRS), I32),
            pltpu.VMEM((BLK, VERT), I32),
            pltpu.SemaphoreType.DMA((2,)),
        ],
        cost_estimate=cost(4e6),
        compiler_params=pltpu.CompilerParams(vmem_limit_bytes=8 * 1024 * 1024),
        name="indices",
    )(in_hbm(pairs), in_hbm(home.reshape(BLK, VERT)))


def whole(*shape):
    return pl.BlockSpec(shape, lambda i, *_: (0,) * len(shape))


def slot(*shape):
    return pl.BlockSpec((1,) + shape, lambda i, *_: (i,) + (0,) * len(shape))


def grid_spec(prefetch, steps, in_specs, out_specs, scratch):
    return pltpu.PrefetchScalarGridSpec(
        num_scalar_prefetch=prefetch,
        grid=(steps,),
        in_specs=in_specs,
        out_specs=out_specs,
        scratch_shapes=scratch,
    )


def table_kernel(pos_ref, nrm_ref, area_ref, out_ref):
    out_ref[:, 0:3, :] = pos_ref[...]
    out_ref[:, 3:6, :] = nrm_ref[...] * (area_ref[...] * (-1.0 / math.pi))
    out_ref[:, 6:8, :] = jnp.ones((BLK, 2, VERT), F32)


def source_table(pos, nrm, area):
    return pl.pallas_call(
        table_kernel,
        out_shape=jax.ShapeDtypeStruct((BLK, 8, VERT), F32),
        cost_estimate=cost(1e6),
        compiler_params=pltpu.CompilerParams(vmem_limit_bytes=8 * 1024 * 1024),
        name="source_table",
    )(pos, nrm, area)


def geometry_kernel(req_ref, table, out_ref):
    def put(i, carry):
        out_ref[i] = table[req_ref[i]].astype(BF16)
        return carry

    lax.fori_loop(0, ROWS, put, 0, unroll=8)


def pack_geometry(req, table):
    return pl.pallas_call(
        geometry_kernel,
        grid_spec=grid_spec(1, 1, [whole(BLK, 8, VERT)], whole(ROWS, 8, VERT), []),
        out_shape=jax.ShapeDtypeStruct((ROWS, 8, VERT), BF16),
        cost_estimate=cost(2e6),
        compiler_params=params(8),
        name="pack_geometry",
    )(req, table)


def invert_kernel(req_ref, order_ref, start_ref, at):
    def clear(b, carry):
        start_ref[b] = 0
        return carry

    lax.fori_loop(0, BLK + 1, clear, 0)

    def count(i, carry):
        b = req_ref[i] + 1
        start_ref[b] = start_ref[b] + 1
        return carry

    lax.fori_loop(0, ROWS, count, 0)

    def add(b, total):
        at[b] = total
        total = total + start_ref[b + 1]
        start_ref[b + 1] = total
        return total

    lax.fori_loop(0, BLK, add, 0)

    def place(i, carry):
        b = req_ref[i]
        order_ref[at[b]] = i
        at[b] = at[b] + 1
        return carry

    lax.fori_loop(0, ROWS, place, 0)


def invert(req):
    smem = pl.BlockSpec(memory_space=pltpu.SMEM)
    return pl.pallas_call(
        invert_kernel,
        grid_spec=grid_spec(1, 1, [], [smem, smem], [pltpu.SMEM((BLK,), I32)]),
        out_shape=(
            jax.ShapeDtypeStruct((ROWS,), I32),
            jax.ShapeDtypeStruct((BLK + 1,), I32),
        ),
        cost_estimate=cost(1e7),
        compiler_params=params(8),
        name="invert",
    )(req)


def ends(last):
    last = last.astype(F32)
    zeros = lambda n: jnp.zeros((n, VERT), F32)
    low = jnp.concatenate([last, zeros(32 - REST)], axis=0)
    high = jnp.concatenate([zeros(SECOND), last, zeros(32 - SECOND - REST)], axis=0)
    return low.astype(BF16), high.astype(BF16)


def send_main(slab, b, i, out_ref, sem):
    at = pl.multiple_of((i & 1) * MAIN, MAIN)
    pltpu.make_async_copy(
        slab.at[b, pl.ds(0, MAIN)], out_ref.at[i >> 1, pl.ds(at, MAIN)], sem
    ).start()


def send_ends(req_ref, low, high, both, out_ref, sems):
    def put(d, carry):
        both[d] = low[req_ref[2 * d]] + high[req_ref[2 * d + 1]]
        return carry

    lax.fori_loop(0, DEVS, put, 0, unroll=8)
    tail = pltpu.make_async_copy(
        both.at[:, pl.ds(0, 24)], out_ref.at[:, pl.ds(2 * MAIN, 24)], sems.at[1]
    )
    tail.start()
    main = out_ref.at[:, pl.ds(0, 2 * MAIN)]
    pltpu.make_async_copy(main, main, sems.at[0]).wait()
    tail.wait()


SEND_SCRATCH = [
    pltpu.VMEM((BLK, 32, VERT), BF16),
    pltpu.VMEM((BLK, 32, VERT), BF16),
    pltpu.VMEM((DEVS, 32, VERT), BF16),
    pltpu.SemaphoreType.DMA((2,)),
]


def send_kernel(req_ref, field_ref, out_ref, slab, low, high, both, sems):
    slab[...] = field_ref[:, :MAIN, :]

    def put(d, carry):
        for k in range(CAP):
            send_main(slab, req_ref[2 * d + k], 2 * d + k, out_ref, sems.at[0])
        return carry

    lax.fori_loop(0, DEVS, put, 0, unroll=8)
    for b in range(BLK):
        low[b], high[b] = ends(field_ref[b, MAIN:, :])
    send_ends(req_ref, low, high, both, out_ref, sems)


def pack_field(req, field):
    return pl.pallas_call(
        send_kernel,
        grid_spec=grid_spec(
            1,
            1,
            [whole(BLK, CH, VERT)],
            pl.BlockSpec(memory_space=pltpu.HBM),
            [pltpu.VMEM((BLK, MAIN, VERT), BF16), *SEND_SCRATCH],
        ),
        out_shape=pltpu.HBM((DEVS, WIRE, VERT), BF16),
        cost_estimate=cost(1e7),
        compiler_params=params(8),
        name="pack_field",
    )(req, field)


def thirds(value):
    high = value.astype(BF16).astype(F32)
    rest = value - high
    middle = rest.astype(BF16).astype(F32)
    return high, middle, (rest - middle).astype(BF16).astype(F32)


NEAR_TERMS = ((0, 0), (0, 1), (1, 0), (1, 1), (0, 2), (2, 0))
FAR_TERMS = ((0, 0), (0, 1), (0, 2))


def stack_rows(parts):
    return jnp.concatenate(parts, axis=0)


def source_rows(geo, terms):
    parts = thirds(geo) if len(terms) > 3 else (geo,)
    square = geo[0:1] * geo[0:1] + geo[1:2] * geo[1:2] + geo[2:3] * geo[2:3] + 1.0
    facing = geo[3:4] * geo[0:1] + geo[4:5] * geo[1:2] + geo[5:6] * geo[2:3]
    zero = jnp.zeros((1, VERT), F32)
    alone = stack_rows([*thirds(square), *thirds(facing), zero, zero])
    return stack_rows([*[parts[i] for i, _ in terms], alone]).T.astype(BF16)


def receiver_rows(pos, nrm, terms):
    zero = jnp.zeros((1, VERT), F32)
    zeros3 = jnp.zeros((3, VERT), F32)
    one = jnp.ones((1, VERT), F32)
    square = pos[0:1] * pos[0:1] + pos[1:2] * pos[1:2] + pos[2:3] * pos[2:3]
    facing = nrm[0:1] * pos[0:1] + nrm[1:2] * pos[1:2] + nrm[2:3] * pos[2:3]
    forms = (
        (stack_rows([-2.0 * pos, zeros3, square, zero]), (1.0, 0.0)),
        (stack_rows([nrm, zeros3, -facing, zero]), (0.0, 0.0)),
        (stack_rows([zeros3, -pos, zero, zero]), (0.0, 1.0)),
    )
    out = []
    for rows, (with_square, with_facing) in forms:
        parts = thirds(rows)
        alone = stack_rows([one * with_square] * 3 + [one * with_facing] * 3 + [zero, zero])
        out.append(stack_rows([*[parts[j] for _, j in terms], alone]))
    return jnp.concatenate(out, axis=1).astype(BF16)


def fill_tiles(index_of, count, recv, table, out_ref):
    right = recv[...]
    for j in range(count):
        got = jnp.dot(table[index_of(j)], right, preferred_element_type=F32)
        soft = got[:, :VERT]
        value = jnp.maximum(got[:, VERT : 2 * VERT], 0.0) * jnp.maximum(got[:, 2 * VERT :], 0.0)
        value = value / (soft * soft)
        out_ref[0, j * VERT : (j + 1) * VERT, :] = value.astype(BF16)


def product(left, right):
    return jnp.dot(left, right, preferred_element_type=F32)


def near_kernel(idx_ref, field_ref, pos_ref, nrm_ref, area_ref, tiles_ref, sum_ref, table, recv, rows):
    s = pl.program_id(0)

    @pl.when(s == 0)
    def _():
        def make(t, carry):
            scaled = nrm_ref[t] * (area_ref[t] * (-1.0 / math.pi))
            geo = stack_rows([pos_ref[t], scaled, jnp.ones((2, VERT), F32)])
            table[t] = source_rows(geo, NEAR_TERMS)
            return carry

        lax.fori_loop(0, BLK, make, 0)

    recv[...] = receiver_rows(pos_ref[s], nrm_ref[s], NEAR_TERMS)
    fill_tiles(lambda j: idx_ref[s * PAIRS + j], NEAR, recv, table, tiles_ref)
    for j in range(NEAR):
        rows[:, j * VERT : (j + 1) * VERT] = field_ref[idx_ref[s * PAIRS + j]]
    sum_ref[0] = product(rows[...], tiles_ref[0])


NEAR_K = 8 * (len(NEAR_TERMS) + 1)
FAR_K = 8 * (len(FAR_TERMS) + 1)


def near_first(idx, field, pos, nrm, area):
    return pl.pallas_call(
        near_kernel,
        grid_spec=grid_spec(
            1,
            BLK,
            [whole(BLK, CH, VERT), whole(BLK, 3, VERT), whole(BLK, 3, VERT), whole(BLK, 1, VERT)],
            [slot(NEAR * VERT, VERT), slot(CH, VERT)],
            [
                pltpu.VMEM((BLK, VERT, NEAR_K), BF16),
                pltpu.VMEM((NEAR_K, 3 * VERT), BF16),
                pltpu.VMEM((CH, NEAR * VERT), BF16),
            ],
        ),
        out_shape=(
            pltpu.HBM((BLK, NEAR * VERT, VERT), BF16),
            jax.ShapeDtypeStruct((BLK, CH, VERT), F32),
        ),
        cost_estimate=cost(6e8),
        compiler_params=params(),
        name="near_first",
    )(idx, field, pos, nrm, area)


def near_again_kernel(idx_ref, field_ref, tiles_ref, sum_ref, rows, tiles, sems):
    s = pl.program_id(0)

    def copies(at):
        return pltpu.make_async_copy(tiles_ref.at[at], tiles.at[at], sems.at[at])

    @pl.when(s == 0)
    def _():
        for at in range(BLK):
            copies(at).start()

    copies(s).wait()
    for j in range(NEAR):
        rows[:, j * VERT : (j + 1) * VERT] = field_ref[idx_ref[s * PAIRS + j]]
    sum_ref[0] = product(rows[...], tiles[s])


def near_again(idx, field, tiles):
    return pl.pallas_call(
        near_again_kernel,
        grid_spec=grid_spec(
            1,
            BLK,
            [whole(BLK, CH, VERT), pl.BlockSpec(memory_space=pltpu.HBM)],
            slot(CH, VERT),
            [
                pltpu.VMEM((CH, NEAR * VERT), BF16),
                pltpu.VMEM((BLK, NEAR * VERT, VERT), BF16),
                pltpu.SemaphoreType.DMA((BLK,)),
            ],
        ),
        out_shape=jax.ShapeDtypeStruct((BLK, CH, VERT), F32),
        cost_estimate=cost(3e8),
        compiler_params=params(),
        name="near_again",
    )(idx, field, in_hbm(tiles))


def far_tiles_kernel(idx_ref, got_ref, pos_ref, nrm_ref, tiles_ref, table, recv):
    s = pl.program_id(0)

    @pl.when(s == 0)
    def _():
        def make(t, carry):
            table[t] = source_rows(got_ref[t].astype(F32), FAR_TERMS)
            return carry

        lax.fori_loop(0, ROWS, make, 0, unroll=4)

    recv[...] = receiver_rows(pos_ref[s], nrm_ref[s], FAR_TERMS)
    fill_tiles(lambda j: idx_ref[s * PAIRS + NEAR + j], FAR, recv, table, tiles_ref)


def far_tiles(idx, got, pos, nrm):
    return pl.pallas_call(
        far_tiles_kernel,
        grid_spec=grid_spec(
            1,
            BLK,
            [whole(ROWS, 8, VERT), whole(BLK, 3, VERT), whole(BLK, 3, VERT)],
            slot(FAR * VERT, VERT),
            [pltpu.VMEM((ROWS, VERT, FAR_K), BF16), pltpu.VMEM((FAR_K, 3 * VERT), BF16)],
        ),
        out_shape=pltpu.HBM((BLK, FAR * VERT, VERT), BF16),
        cost_estimate=cost(6e8),
        compiler_params=params(),
        name="far_tiles",
    )(idx, got, pos, nrm)


def far_kernel(
    idx_ref,
    req_ref,
    order_ref,
    start_ref,
    got_ref,
    tiles_ref,
    near_ref,
    albedo_ref,
    area_ref,
    out_ref,
    energy_ref,
    *more,
    send,
):
    if send:
        wire_ref, rows, field, last, tiles, sems, slab, low, high, both, out_sems = more
    else:
        rows, field, last, tiles, sems = more
    ahead = 3
    arrived = pltpu.make_async_copy(got_ref, field.at[:, pl.ds(0, WIRE)], sems.at[BLK])
    arrived.start()

    def copies(at):
        return pltpu.make_async_copy(tiles_ref.at[at], tiles.at[at], sems.at[at])

    for at in range(ahead):
        copies(at).start()
    arrived.wait()
    for at in range(ahead, BLK):
        copies(at).start()

    def split(d, carry):
        both_ends = field[d, 2 * MAIN : 2 * MAIN + 32]
        last[2 * d] = both_ends[0:16]
        last[2 * d + 1] = both_ends[SECOND : SECOND + 16]
        return carry

    lax.fori_loop(0, DEVS, split, 0, unroll=8)
    channel = lax.broadcasted_iota(I32, (CH, VERT), 0)

    def gather(s, rows):
        for j in range(FAR):
            row = idx_ref[s * PAIRS + NEAR + j]
            cols = slice(j * VERT, (j + 1) * VERT)
            at = pl.multiple_of((row & 1) * MAIN, MAIN)
            rows[0:MAIN, cols] = field[row >> 1, pl.ds(at, MAIN)]
            rows[MAIN : MAIN + 16, cols] = last[row]

    def finish(s, got):
        total = near_ref[s] + got[:CH]
        shade = jnp.where(
            channel < CH // COLORS,
            albedo_ref[s, 0:1, :],
            jnp.where(channel < 2 * (CH // COLORS), albedo_ref[s, 1:2, :], albedo_ref[s, 2:3, :]),
        )
        bounce = total * shade
        rounded = bounce.astype(BF16)
        out_ref[s] = rounded
        if send:
            slab[s] = rounded[:MAIN]
            low[s], high[s] = ends(rounded[MAIN:])
        return jnp.sum(area_ref[s] * bounce * bounce, axis=0, keepdims=True)

    def group(h, energy):
        these = [h * GROUP + i for i in range(GROUP)]
        for s in these:
            copies(s).wait()
        for i, s in enumerate(these):
            gather(s, rows.at[i])
        results = [product(rows[i], tiles[s]) for i, s in enumerate(these)]
        for s, got in zip(these, results):
            energy = energy + finish(s, got)
        if send:

            def push(i, carry):
                send_main(slab, req_ref[order_ref[i]], order_ref[i], wire_ref, out_sems.at[0])
                return carry

            lax.fori_loop(start_ref[h * GROUP], start_ref[(h + 1) * GROUP], push, 0)
        return energy

    energy_ref[...] = lax.fori_loop(0, BLK // GROUP, group, jnp.zeros((1, VERT), F32))
    if send:
        send_ends(req_ref, low, high, both, wire_ref, out_sems)


GROUP = 2


def far_bounce(idx, req, order, start, got, tiles, near, albedo, area, send):
    hbm = pl.BlockSpec(memory_space=pltpu.HBM)
    return pl.pallas_call(
        functools.partial(far_kernel, send=send),
        grid_spec=grid_spec(
            4,
            1,
            [hbm, hbm, whole(BLK, CH, VERT), whole(BLK, COLORS, VERT), whole(BLK, 1, VERT)],
            [whole(BLK, CH, VERT), whole(1, VERT)] + [hbm] * send,
            [
                pltpu.VMEM((GROUP, MAIN + 16, FAR * VERT), BF16),
                pltpu.VMEM((DEVS, WIRE + 8, VERT), BF16),
                pltpu.VMEM((ROWS, 16, VERT), BF16),
                pltpu.VMEM((BLK, FAR * VERT, VERT), BF16),
                pltpu.SemaphoreType.DMA((BLK + 1,)),
            ]
            + [pltpu.VMEM((BLK, MAIN, VERT), BF16), *SEND_SCRATCH] * send,
        ),
        out_shape=[
            jax.ShapeDtypeStruct((BLK, CH, VERT), BF16),
            jax.ShapeDtypeStruct((1, VERT), F32),
        ]
        + [pltpu.HBM((DEVS, WIRE, VERT), BF16)] * send,
        cost_estimate=cost(5e8),
        compiler_params=params(),
        name="far_bounce_one" if send else "far_bounce_two",
    )(idx, req, order, start, in_hbm(got), in_hbm(tiles), near, albedo, area)


def swap(value):
    return lax.all_to_all(value, AXES, split_axis=0, concat_axis=0, tiled=True)


def body(transfer, positions, normals, area, albedo, pairs, home):
    area_row = area.reshape(BLK, 1, VERT)
    idx, need = find_indices(pairs, home)
    idx = idx.reshape(-1)
    sources = source_table(positions, normals, area_row)
    asked = swap(need).reshape(-1)
    geometry = swap(pack_geometry(asked, sources))
    got_one = swap(pack_field(asked, transfer))
    near_tiles, near_one = near_first(idx, transfer, positions, normals, area_row)
    tiles = far_tiles(idx, geometry, positions, normals)
    lists = invert(asked)
    bounce_one, share_one, wire = far_bounce(
        idx, asked, *lists, got_one, tiles, near_one, albedo, area_row, True
    )
    got_two = swap(wire)
    near_two = near_again(idx, bounce_one, near_tiles)
    bounce_two, share_two = far_bounce(
        idx, asked, *lists, got_two, tiles, near_two, albedo, area_row, False
    )
    shares = jnp.concatenate([share_one, share_two], axis=0)
    shares = swap(jnp.broadcast_to(shares[None], (DEVS, 2, VERT)))
    energies = jnp.sum(shares, axis=(0, 2)) * (1.0 / (DEVS * BLK * VERT * CH))
    return bounce_one, bounce_two, energies


def solution(mesh):
    finer = Mesh(mesh.devices.reshape(4, 2, 4, 4), AXES)
    three = P(AXES, None, None)
    return jax.shard_map(
        body,
        mesh=finer,
        in_specs=(three, three, three, P(AXES, None), three, P(AXES, None), P()),
        out_specs=(three, three, P()),
        check_vma=False,
    )
```

```python
import functools
import math

import jax
import jax.numpy as jnp
from jax import lax
from jax.experimental import pallas as pl
from jax.experimental.pallas import tpu as pltpu
from jax.sharding import Mesh
from jax.sharding import PartitionSpec as P

COLORS = 3
NEAR = 16
FAR = 24
PAIRS = NEAR + FAR
CAP = 2
CH = 75
MAIN = 64
REST = CH - MAIN
SECOND = 12
WIRE = 2 * MAIN + 24
BLK = 16
VERT = 128
DEVS = 128
ROWS = DEVS * CAP
AXES = ("gx_0", "gx_1", "gy_0", "gy_1")

F32 = jnp.float32
BF16 = jnp.bfloat16
I32 = jnp.int32


def in_hbm(value):
    return pltpu.with_memory_space_constraint(value, pltpu.HBM)


def params(limit_mib=40):
    return pltpu.CompilerParams(
        dimension_semantics=("arbitrary",), vmem_limit_bytes=limit_mib * 1024 * 1024
    )


def cost(flops, read=0):
    return pl.CostEstimate(flops=int(flops), bytes_accessed=int(read), transcendentals=0)


def index_kernel(pairs_hbm, home_hbm, idx_ref, req_ref, pairs_ref, home_ref, sems):
    first = pltpu.make_async_copy(pairs_hbm, pairs_ref, sems.at[0])
    second = pltpu.make_async_copy(home_hbm, home_ref, sems.at[1])
    first.start()
    second.start()
    first.wait()
    second.wait()
    home = home_ref[...]
    both = jnp.concatenate([home >> 4, home & 15], axis=0).astype(F32).astype(BF16)
    pairs = pairs_ref[...]
    low = pairs & 127
    high = pairs >> 7
    sub = lax.broadcasted_iota(I32, (VERT, PAIRS), 0)
    sub_f = sub.astype(F32)
    sub16 = lax.broadcasted_iota(I32, (16, PAIRS), 0)
    lane = lax.broadcasted_iota(I32, (VERT, PAIRS), 1)
    lane_row = lax.broadcasted_iota(I32, (1, PAIRS), 1)
    is_far = lane >= NEAR
    owners, locals_ = [], []
    least = jnp.full((VERT, PAIRS), 99.0, F32)
    most = jnp.full((VERT, PAIRS), -1.0, F32)
    for s in range(BLK):
        hot = jnp.where(sub == low[s : s + 1, :], 1.0, 0.0).astype(BF16)
        got = jnp.dot(both, hot, preferred_element_type=F32)
        here = sub16 == high[s : s + 1, :]
        owner = jnp.sum(jnp.where(here, got[:16], 0.0), axis=0, keepdims=True)
        local = jnp.sum(jnp.where(here, got[16:], 0.0), axis=0, keepdims=True)
        owners.append(owner)
        locals_.append(local)
        same = (sub_f == owner) & is_far
        least = jnp.minimum(least, jnp.where(same, local, 99.0))
        most = jnp.maximum(most, jnp.where(same, local, -1.0))
    lo = jnp.min(least, axis=1, keepdims=True)
    hi = jnp.max(most, axis=1, keepdims=True)
    for s in range(BLK):
        first = jnp.sum(jnp.where(sub_f == owners[s], lo, 0.0), axis=0, keepdims=True)
        far_row = owners[s] * 2.0 + jnp.where(locals_[s] == first, 0.0, 1.0)
        idx_ref[s : s + 1, :] = jnp.where(lane_row < NEAR, locals_[s], far_row).astype(I32)
    used = hi >= 0.0
    req_ref[:, 0:1] = jnp.where(used, lo, 0.0).astype(I32)
    req_ref[:, 1:2] = jnp.where(used, hi, 0.0).astype(I32)


def find_indices(pairs, home):
    return pl.pallas_call(
        index_kernel,
        out_shape=(
            jax.ShapeDtypeStruct((BLK, PAIRS), I32),
            jax.ShapeDtypeStruct((DEVS, CAP), I32),
        ),
        in_specs=[pl.BlockSpec(memory_space=pltpu.HBM), pl.BlockSpec(memory_space=pltpu.HBM)],
        scratch_shapes=[
            pltpu.VMEM((BLK, PAIRS), I32),
            pltpu.VMEM((BLK, VERT), I32),
            pltpu.SemaphoreType.DMA((2,)),
        ],
        cost_estimate=cost(4e6),
        compiler_params=pltpu.CompilerParams(vmem_limit_bytes=8 * 1024 * 1024),
        name="indices",
    )(in_hbm(pairs), in_hbm(home.reshape(BLK, VERT)))


def whole(*shape):
    return pl.BlockSpec(shape, lambda i, *_: (0,) * len(shape))


def slot(*shape):
    return pl.BlockSpec((1,) + shape, lambda i, *_: (i,) + (0,) * len(shape))


def grid_spec(prefetch, steps, in_specs, out_specs, scratch):
    return pltpu.PrefetchScalarGridSpec(
        num_scalar_prefetch=prefetch,
        grid=(steps,),
        in_specs=in_specs,
        out_specs=out_specs,
        scratch_shapes=scratch,
    )


def table_kernel(pos_ref, nrm_ref, area_ref, out_ref):
    scaled = nrm_ref[...] * (area_ref[...] * (-1.0 / math.pi))
    for i in range(3):
        both = jnp.concatenate([pos_ref[:, i : i + 1, :], scaled[:, i : i + 1, :]], axis=1)
        out_ref[:, i] = both.astype(BF16)


def source_table(pos, nrm, area):
    return pl.pallas_call(
        table_kernel,
        out_shape=jax.ShapeDtypeStruct((BLK, 3, 2, VERT), BF16),
        cost_estimate=cost(1e6),
        compiler_params=pltpu.CompilerParams(vmem_limit_bytes=8 * 1024 * 1024),
        name="source_table",
    )(pos, nrm, area)


def geometry_kernel(req_ref, table, out_ref):
    def put(d, carry):
        for k in range(CAP):
            out_ref[d, :, 2 * k : 2 * k + 2, :] = table[req_ref[d, 0, k]]
        return carry

    lax.fori_loop(0, DEVS, put, 0, unroll=8)


def pack_geometry(req, table):
    return pl.pallas_call(
        geometry_kernel,
        grid_spec=grid_spec(1, 1, [whole(BLK, 3, 2, VERT)], whole(DEVS, 3, 4, VERT), []),
        out_shape=jax.ShapeDtypeStruct((DEVS, 3, 4, VERT), BF16),
        cost_estimate=cost(2e6),
        compiler_params=params(8),
        name="pack_geometry",
    )(req, table)


def ends(last):
    last = last.astype(F32)
    zeros = lambda n: jnp.zeros((n, VERT), F32)
    low = jnp.concatenate([last, zeros(32 - REST)], axis=0)
    high = jnp.concatenate([zeros(SECOND), last, zeros(32 - SECOND - REST)], axis=0)
    return low.astype(BF16), high.astype(BF16)


def send_all(req_ref, slab, low, high, both, out_ref, sems):
    def main_rows(d, carry):
        for k in range(CAP):
            pltpu.make_async_copy(
                slab.at[req_ref[2 * d + k]], out_ref.at[d, pl.ds(k * MAIN, MAIN)], sems.at[0]
            ).start()
        return carry

    lax.fori_loop(0, DEVS, main_rows, 0, unroll=16)

    def put(d, carry):
        both[d] = low[req_ref[2 * d]] + high[req_ref[2 * d + 1]]
        return carry

    lax.fori_loop(0, DEVS, put, 0, unroll=8)
    tail = pltpu.make_async_copy(
        both.at[:, pl.ds(0, 24)], out_ref.at[:, pl.ds(2 * MAIN, 24)], sems.at[1]
    )
    tail.start()
    main = out_ref.at[:, pl.ds(0, 2 * MAIN)]
    pltpu.make_async_copy(main, main, sems.at[0]).wait()
    tail.wait()


SEND_SCRATCH = [
    pltpu.VMEM((BLK, 32, VERT), BF16),
    pltpu.VMEM((BLK, 32, VERT), BF16),
    pltpu.VMEM((DEVS, 32, VERT), BF16),
    pltpu.SemaphoreType.DMA((2,)),
]


def send_kernel(req_ref, field_ref, out_ref, slab, low, high, both, sems):
    slab[...] = field_ref[:, :MAIN, :]
    for b in range(BLK):
        low[b], high[b] = ends(field_ref[b, MAIN:, :])
    send_all(req_ref, slab, low, high, both, out_ref, sems)


def pack_field(req, field):
    return pl.pallas_call(
        send_kernel,
        grid_spec=grid_spec(
            1,
            1,
            [whole(BLK, CH, VERT)],
            pl.BlockSpec(memory_space=pltpu.HBM),
            [pltpu.VMEM((BLK, MAIN, VERT), BF16), *SEND_SCRATCH],
        ),
        out_shape=pltpu.HBM((DEVS, WIRE, VERT), BF16),
        cost_estimate=cost(1e7),
        compiler_params=params(8),
        name="pack_field",
    )(req, field)


def thirds(value):
    high = value.astype(BF16).astype(F32)
    rest = value - high
    middle = rest.astype(BF16).astype(F32)
    return high, middle, (rest - middle).astype(BF16).astype(F32)


NEAR_TERMS = ((0, 0), (0, 1), (1, 0), (1, 1), (0, 2), (2, 0))
FAR_TERMS = ((0, 0), (0, 1), (0, 2))


def stack_rows(parts):
    return jnp.concatenate(parts, axis=0)


def source_rows(geo, terms):
    parts = thirds(geo) if len(terms) > 3 else (geo,)
    square = geo[0:1] * geo[0:1] + geo[1:2] * geo[1:2] + geo[2:3] * geo[2:3] + 1.0
    facing = geo[3:4] * geo[0:1] + geo[4:5] * geo[1:2] + geo[5:6] * geo[2:3]
    zero = jnp.zeros((1, VERT), F32)
    alone = stack_rows([*thirds(square), *thirds(facing), zero, zero])
    return stack_rows([*[parts[i] for i, _ in terms], alone]).T.astype(BF16)


def receiver_rows(pos, nrm, terms):
    zero = jnp.zeros((1, VERT), F32)
    zeros3 = jnp.zeros((3, VERT), F32)
    one = jnp.ones((1, VERT), F32)
    square = pos[0:1] * pos[0:1] + pos[1:2] * pos[1:2] + pos[2:3] * pos[2:3]
    facing = nrm[0:1] * pos[0:1] + nrm[1:2] * pos[1:2] + nrm[2:3] * pos[2:3]
    forms = (
        (stack_rows([-2.0 * pos, zeros3, square, zero]), (1.0, 0.0)),
        (stack_rows([nrm, zeros3, -facing, zero]), (0.0, 0.0)),
        (stack_rows([zeros3, -pos, zero, zero]), (0.0, 1.0)),
    )
    out = []
    for rows, (with_square, with_facing) in forms:
        parts = thirds(rows)
        alone = stack_rows([one * with_square] * 3 + [one * with_facing] * 3 + [zero, zero])
        out.append(stack_rows([*[parts[j] for _, j in terms], alone]))
    return jnp.concatenate(out, axis=1).astype(BF16)


def fill_tiles(index_of, count, recv, table, out_ref):
    right = recv[...]
    for j in range(count):
        got = jnp.dot(table[index_of(j)], right, preferred_element_type=F32)
        soft = got[:, :VERT]
        value = jnp.maximum(got[:, VERT : 2 * VERT], 0.0) * jnp.maximum(got[:, 2 * VERT :], 0.0)
        value = value / (soft * soft)
        out_ref[0, j * VERT : (j + 1) * VERT, :] = value.astype(BF16)


def product(left, right):
    return jnp.dot(left, right, preferred_element_type=F32)


def near_kernel(idx_ref, field_ref, pos_ref, nrm_ref, area_ref, tiles_ref, sum_ref, table, recv, rows):
    s = pl.program_id(0)

    @pl.when(s == 0)
    def _():
        def make(t, carry):
            scaled = nrm_ref[t] * (area_ref[t] * (-1.0 / math.pi))
            geo = stack_rows([pos_ref[t], scaled, jnp.ones((2, VERT), F32)])
            table[t] = source_rows(geo, NEAR_TERMS)
            return carry

        lax.fori_loop(0, BLK, make, 0)

    recv[...] = receiver_rows(pos_ref[s], nrm_ref[s], NEAR_TERMS)
    fill_tiles(lambda j: idx_ref[s * PAIRS + j], NEAR, recv, table, tiles_ref)
    for j in range(NEAR):
        rows[:, j * VERT : (j + 1) * VERT] = field_ref[idx_ref[s * PAIRS + j]]
    sum_ref[0] = product(rows[...], tiles_ref[0])


NEAR_K = 8 * (len(NEAR_TERMS) + 1)
FAR_K = 8 * (len(FAR_TERMS) + 1)


def near_first(idx, field, pos, nrm, area):
    return pl.pallas_call(
        near_kernel,
        grid_spec=grid_spec(
            1,
            BLK,
            [whole(BLK, CH, VERT), whole(BLK, 3, VERT), whole(BLK, 3, VERT), whole(BLK, 1, VERT)],
            [slot(NEAR * VERT, VERT), slot(CH, VERT)],
            [
                pltpu.VMEM((BLK, VERT, NEAR_K), BF16),
                pltpu.VMEM((NEAR_K, 3 * VERT), BF16),
                pltpu.VMEM((CH, NEAR * VERT), BF16),
            ],
        ),
        out_shape=(
            pltpu.HBM((BLK, NEAR * VERT, VERT), BF16),
            jax.ShapeDtypeStruct((BLK, CH, VERT), F32),
        ),
        cost_estimate=cost(6e8),
        compiler_params=params(),
        name="near_first",
    )(idx, field, pos, nrm, area)


def near_again_kernel(idx_ref, field_ref, tiles_ref, sum_ref, rows, tiles, sems):
    s = pl.program_id(0)

    def copies(at):
        return pltpu.make_async_copy(tiles_ref.at[at], tiles.at[at], sems.at[at])

    @pl.when(s == 0)
    def _():
        for at in range(BLK):
            copies(at).start()

    copies(s).wait()
    for j in range(NEAR):
        rows[:, j * VERT : (j + 1) * VERT] = field_ref[idx_ref[s * PAIRS + j]]
    sum_ref[0] = product(rows[...], tiles[s])


def near_again(idx, field, tiles):
    return pl.pallas_call(
        near_again_kernel,
        grid_spec=grid_spec(
            1,
            BLK,
            [whole(BLK, CH, VERT), pl.BlockSpec(memory_space=pltpu.HBM)],
            slot(CH, VERT),
            [
                pltpu.VMEM((CH, NEAR * VERT), BF16),
                pltpu.VMEM((BLK, NEAR * VERT, VERT), BF16),
                pltpu.SemaphoreType.DMA((BLK,)),
            ],
        ),
        out_shape=jax.ShapeDtypeStruct((BLK, CH, VERT), F32),
        cost_estimate=cost(3e8),
        compiler_params=params(),
        name="near_again",
    )(idx, field, in_hbm(tiles))


def far_tiles_kernel(idx_ref, got_ref, pos_ref, nrm_ref, tiles_ref, table, recv):
    s = pl.program_id(0)

    @pl.when(s == 0)
    def _():
        def make(d, carry):
            got = [got_ref[d, i].astype(F32) for i in range(3)]
            ones = jnp.ones((2, VERT), F32)
            for k in range(CAP):
                parts = [g[2 * k : 2 * k + 1] for g in got] + [g[2 * k + 1 : 2 * k + 2] for g in got]
                table[CAP * d + k] = source_rows(stack_rows([*parts, ones]), FAR_TERMS)
            return carry

        lax.fori_loop(0, DEVS, make, 0, unroll=2)

    recv[...] = receiver_rows(pos_ref[s], nrm_ref[s], FAR_TERMS)
    fill_tiles(lambda j: idx_ref[s * PAIRS + NEAR + j], FAR, recv, table, tiles_ref)


def far_tiles(idx, got, pos, nrm):
    return pl.pallas_call(
        far_tiles_kernel,
        grid_spec=grid_spec(
            1,
            BLK,
            [whole(DEVS, 3, 4, VERT), whole(BLK, 3, VERT), whole(BLK, 3, VERT)],
            slot(FAR * VERT, VERT),
            [pltpu.VMEM((ROWS, VERT, FAR_K), BF16), pltpu.VMEM((FAR_K, 3 * VERT), BF16)],
        ),
        out_shape=pltpu.HBM((BLK, FAR * VERT, VERT), BF16),
        cost_estimate=cost(6e8),
        compiler_params=params(),
        name="far_tiles",
    )(idx, got, pos, nrm)


def far_kernel(
    idx_any,
    req_any,
    got_ref,
    tiles_ref,
    near_ref,
    albedo_ref,
    area_ref,
    share_ref,
    out_ref,
    energy_ref,
    *more,
    send,
):
    if send:
        wire_ref, idx_ref, req_ref, rows, field, last, tiles, sems, slab, low, high, both, out_sems = more
    else:
        idx_ref, req_ref, rows, field, last, tiles, sems = more
    ahead = 3
    arrived = pltpu.make_async_copy(got_ref, field.at[:, pl.ds(0, WIRE)], sems.at[BLK])
    arrived.start()

    def copies(at):
        return pltpu.make_async_copy(tiles_ref.at[at], tiles.at[at], sems.at[at])

    small = [pltpu.make_async_copy(idx_any, idx_ref, sems.at[BLK + 1])]
    if send:
        small.append(pltpu.make_async_copy(req_any, req_ref, sems.at[BLK + 2]))
    for one in small:
        one.start()
    for at in range(ahead):
        copies(at).start()
    for one in small:
        one.wait()
    arrived.wait()
    for at in range(ahead, BLK):
        copies(at).start()

    def split(d, carry):
        both_ends = field[d, 2 * MAIN : 2 * MAIN + 32]
        last[2 * d] = both_ends[0:16]
        last[2 * d + 1] = both_ends[SECOND : SECOND + 16]
        return carry

    lax.fori_loop(0, DEVS, split, 0, unroll=8)
    channel = lax.broadcasted_iota(I32, (CH, VERT), 0)

    def gather(s, rows):
        for j in range(FAR):
            row = idx_ref[s * PAIRS + NEAR + j]
            cols = slice(j * VERT, (j + 1) * VERT)
            at = pl.multiple_of((row & 1) * MAIN, MAIN)
            rows[0:MAIN, cols] = field[row >> 1, pl.ds(at, MAIN)]
            rows[MAIN : MAIN + 16, cols] = last[row]

    def finish(s, got):
        total = near_ref[s] + got[:CH]
        shade = jnp.where(
            channel < CH // COLORS,
            albedo_ref[s, 0:1, :],
            jnp.where(channel < 2 * (CH // COLORS), albedo_ref[s, 1:2, :], albedo_ref[s, 2:3, :]),
        )
        bounce = total * shade
        rounded = bounce.astype(BF16)
        out_ref[s] = rounded
        if send:
            slab[s] = rounded[:MAIN]
            low[s], high[s] = ends(rounded[MAIN:])
        return jnp.sum(area_ref[s] * bounce * bounce, axis=0, keepdims=True)

    def group(h, energy):
        these = [h * GROUP + i for i in range(GROUP)]
        for s in these:
            copies(s).wait()
        for i, s in enumerate(these):
            gather(s, rows.at[i])
        results = [product(rows[i], tiles[s]) for i, s in enumerate(these)]
        for s, got in zip(these, results):
            energy = energy + finish(s, got)
        return energy

    energy = lax.fori_loop(0, BLK // GROUP, group, jnp.zeros((1, VERT), F32)) * INV_COUNT
    if send:
        energy_ref[...] = energy
        send_all(req_ref, slab, low, high, both, wire_ref, out_sems)
    else:
        shares = jnp.concatenate([share_ref[...], energy], axis=0)
        energy_ref[...] = jnp.broadcast_to(shares[None], (DEVS, 2, VERT))


GROUP = 2
INV_COUNT = 1.0 / (DEVS * BLK * VERT * CH)


def far_bounce(idx, req, got, tiles, near, albedo, area, share, send):
    hbm = pl.BlockSpec(memory_space=pltpu.HBM)
    vmem = pl.BlockSpec(memory_space=pltpu.VMEM)
    any_space = pl.BlockSpec(memory_space=pl.ANY)
    return pl.pallas_call(
        functools.partial(far_kernel, send=send),
        grid_spec=grid_spec(
            0,
            1,
            [any_space, any_space, hbm, hbm, vmem, vmem, vmem, vmem],
            [vmem, vmem] + [hbm] * send,
            [
                pltpu.SMEM((BLK * PAIRS,), I32),
                pltpu.SMEM((ROWS,), I32),
                pltpu.VMEM((GROUP, MAIN + 16, FAR * VERT), BF16),
                pltpu.VMEM((DEVS, WIRE + 8, VERT), BF16),
                pltpu.VMEM((ROWS, 16, VERT), BF16),
                pltpu.VMEM((BLK, FAR * VERT, VERT), BF16),
                pltpu.SemaphoreType.DMA((BLK + 3,)),
            ]
            + [pltpu.VMEM((BLK, MAIN, VERT), BF16), *SEND_SCRATCH] * send,
        ),
        out_shape=[
            jax.ShapeDtypeStruct((BLK, CH, VERT), BF16),
            jax.ShapeDtypeStruct((1, VERT) if send else (DEVS, 2, VERT), F32),
        ]
        + [pltpu.HBM((DEVS, WIRE, VERT), BF16)] * send,
        cost_estimate=cost(5e8),
        compiler_params=params(),
        name="far_bounce_one" if send else "far_bounce_two",
    )(idx, req, in_hbm(got), in_hbm(tiles), near, albedo, area, share)


def swap(value):
    return lax.all_to_all(value, AXES, split_axis=0, concat_axis=0, tiled=True)


def body(transfer, positions, normals, area, albedo, pairs, home):
    area_row = area.reshape(BLK, 1, VERT)
    idx, need = find_indices(pairs, home)
    idx = idx.reshape(-1)
    sources = source_table(positions, normals, area_row)
    asked = swap(need.reshape(DEVS, 1, CAP))
    geometry = swap(pack_geometry(asked, sources))
    asked = asked.reshape(-1)
    got_one = swap(pack_field(asked, transfer))
    near_tiles, near_one = near_first(idx, transfer, positions, normals, area_row)
    tiles = far_tiles(idx, geometry, positions, normals)
    none = jnp.zeros((1, VERT), F32)
    bounce_one, share_one, wire = far_bounce(
        idx, asked, got_one, tiles, near_one, albedo, area_row, none, True
    )
    got_two = swap(wire)
    near_two = near_again(idx, bounce_one, near_tiles)
    bounce_two, shares = far_bounce(
        idx, asked, got_two, tiles, near_two, albedo, area_row, share_one, False
    )
    energies = jnp.sum(swap(shares), axis=(0, 2))
    return bounce_one, bounce_two, energies


def solution(mesh):
    finer = Mesh(mesh.devices.reshape(4, 2, 4, 4), AXES)
    three = P(AXES, None, None)
    return jax.shard_map(
        body,
        mesh=finer,
        in_specs=(three, three, three, P(AXES, None), three, P(AXES, None), P()),
        out_specs=(three, three, P()),
        check_vma=False,
    )
```

```python
import functools
import math

import jax
import jax.numpy as jnp
from jax import lax
from jax.experimental import pallas as pl
from jax.experimental.pallas import tpu as pltpu
from jax.sharding import Mesh
from jax.sharding import PartitionSpec as P

COLORS = 3
NEAR = 16
FAR = 24
PAIRS = NEAR + FAR
CAP = 2
CH = 75
MAIN = 64
REST = CH - MAIN
SECOND = 12
WIRE = 2 * MAIN + 24
BLK = 16
VERT = 128
DEVS = 128
ROWS = DEVS * CAP
AXES = ("gx_0", "gx_1", "gy_0", "gy_1")

F32 = jnp.float32
BF16 = jnp.bfloat16
I32 = jnp.int32


def in_hbm(value):
    return pltpu.with_memory_space_constraint(value, pltpu.HBM)


def params(limit_mib=40):
    return pltpu.CompilerParams(
        dimension_semantics=("arbitrary",), vmem_limit_bytes=limit_mib * 1024 * 1024
    )


def cost(flops, read=0):
    return pl.CostEstimate(flops=int(flops), bytes_accessed=int(read), transcendentals=0)


TOGETHER = 4


def home_parts(home):
    return jnp.concatenate([home >> 4, home & 15], axis=0).astype(F32).astype(BF16)


def look_up(both, blocks):
    wide = blocks.shape[1]
    sub = lax.broadcasted_iota(I32, (VERT, wide), 0)
    hot = jnp.where(sub == (blocks & 127), 1.0, 0.0).astype(BF16)
    got = jnp.dot(both, hot, preferred_element_type=F32)
    here = lax.broadcasted_iota(I32, (16, wide), 0) == (blocks >> 7)
    owner = jnp.sum(jnp.where(here, got[:16], 0.0), axis=0, keepdims=True)
    local = jnp.sum(jnp.where(here, got[16:], 0.0), axis=0, keepdims=True)
    return owner, local


def request_kernel(pairs_hbm, home_hbm, req_ref, pairs_ref, home_ref, sems):
    first = pltpu.make_async_copy(pairs_hbm, pairs_ref, sems.at[0])
    second = pltpu.make_async_copy(home_hbm, home_ref, sems.at[1])
    first.start()
    second.start()
    first.wait()
    second.wait()
    both = home_parts(home_ref[...])
    far = pairs_ref[...][:, NEAR:]
    wide = TOGETHER * FAR
    device = lax.broadcasted_iota(I32, (VERT, wide), 0).astype(F32)
    least = jnp.full((VERT, wide), 99.0, F32)
    most = jnp.full((VERT, wide), -1.0, F32)
    for g in range(BLK // TOGETHER):
        rows = [far[g * TOGETHER + i : g * TOGETHER + i + 1] for i in range(TOGETHER)]
        owner, local = look_up(both, jnp.concatenate(rows, axis=1))
        same = device == owner
        least = jnp.minimum(least, jnp.where(same, local, 99.0))
        most = jnp.maximum(most, jnp.where(same, local, -1.0))
    lo = jnp.min(least, axis=1, keepdims=True)
    hi = jnp.max(most, axis=1, keepdims=True)
    used = hi >= 0.0
    req_ref[:, 0:1] = jnp.where(used, lo, 0.0).astype(I32)
    req_ref[:, 1:2] = jnp.where(used, hi, 0.0).astype(I32)


def find_requests(pairs, home):
    return pl.pallas_call(
        request_kernel,
        out_shape=jax.ShapeDtypeStruct((DEVS, CAP), I32),
        in_specs=[pl.BlockSpec(memory_space=pltpu.HBM), pl.BlockSpec(memory_space=pltpu.HBM)],
        scratch_shapes=[
            pltpu.VMEM((BLK, PAIRS), I32),
            pltpu.VMEM((BLK, VERT), I32),
            pltpu.SemaphoreType.DMA((2,)),
        ],
        cost_estimate=cost(2e6),
        compiler_params=pltpu.CompilerParams(vmem_limit_bytes=8 * 1024 * 1024),
        name="requests",
    )(in_hbm(pairs), in_hbm(home))


def index_kernel(pairs_ref, home_ref, req_ref, idx_ref):
    both = home_parts(home_ref[...])
    pairs = pairs_ref[...]
    device = lax.broadcasted_iota(I32, (VERT, PAIRS), 0).astype(F32)
    lane = lax.broadcasted_iota(I32, (1, PAIRS), 1)
    lo = req_ref[:, 0:1].astype(F32)
    for s in range(BLK):
        owner, local = look_up(both, pairs[s : s + 1, :])
        first = jnp.sum(jnp.where(device == owner, lo, 0.0), axis=0, keepdims=True)
        far_row = owner * 2.0 + jnp.where(local == first, 0.0, 1.0)
        idx_ref[s : s + 1, :] = jnp.where(lane < NEAR, local, far_row).astype(I32)


def find_indices(pairs, home, need):
    return pl.pallas_call(
        index_kernel,
        out_shape=jax.ShapeDtypeStruct((BLK, PAIRS), I32),
        cost_estimate=cost(4e6),
        compiler_params=pltpu.CompilerParams(vmem_limit_bytes=8 * 1024 * 1024),
        name="indices",
    )(pairs, home, need)


def whole(*shape):
    return pl.BlockSpec(shape, lambda i, *_: (0,) * len(shape))


def slot(*shape):
    return pl.BlockSpec((1,) + shape, lambda i, *_: (i,) + (0,) * len(shape))


def grid_spec(prefetch, steps, in_specs, out_specs, scratch):
    return pltpu.PrefetchScalarGridSpec(
        num_scalar_prefetch=prefetch,
        grid=(steps,),
        in_specs=in_specs,
        out_specs=out_specs,
        scratch_shapes=scratch,
    )


def table_kernel(pos_ref, nrm_ref, area_ref, out_ref):
    scaled = nrm_ref[...] * (area_ref[...] * (-1.0 / math.pi))
    for i in range(3):
        both = jnp.concatenate([pos_ref[:, i : i + 1, :], scaled[:, i : i + 1, :]], axis=1)
        out_ref[:, i] = both.astype(BF16)


def source_table(pos, nrm, area):
    return pl.pallas_call(
        table_kernel,
        out_shape=jax.ShapeDtypeStruct((BLK, 3, 2, VERT), BF16),
        cost_estimate=cost(1e6),
        compiler_params=pltpu.CompilerParams(vmem_limit_bytes=8 * 1024 * 1024),
        name="source_table",
    )(pos, nrm, area)


def geometry_kernel(req_ref, table, out_ref):
    def put(d, carry):
        for k in range(CAP):
            out_ref[d, :, 2 * k : 2 * k + 2, :] = table[req_ref[d, 0, k]]
        return carry

    lax.fori_loop(0, DEVS, put, 0, unroll=8)


def pack_geometry(req, table):
    return pl.pallas_call(
        geometry_kernel,
        grid_spec=grid_spec(1, 1, [whole(BLK, 3, 2, VERT)], whole(DEVS, 3, 4, VERT), []),
        out_shape=jax.ShapeDtypeStruct((DEVS, 3, 4, VERT), BF16),
        cost_estimate=cost(2e6),
        compiler_params=params(8),
        name="pack_geometry",
    )(req, table)


def ends(last):
    last = last.astype(F32)
    zeros = lambda n: jnp.zeros((n, VERT), F32)
    low = jnp.concatenate([last, zeros(32 - REST)], axis=0)
    high = jnp.concatenate([zeros(SECOND), last, zeros(32 - SECOND - REST)], axis=0)
    return low.astype(BF16), high.astype(BF16)


def send_all(req_ref, slab, low, high, both, out_ref, sems):
    def main_rows(d, carry):
        for k in range(CAP):
            pltpu.make_async_copy(
                slab.at[req_ref[2 * d + k]], out_ref.at[d, pl.ds(k * MAIN, MAIN)], sems.at[0]
            ).start()
        return carry

    lax.fori_loop(0, DEVS, main_rows, 0, unroll=16)

    def put(d, carry):
        both[d] = low[req_ref[2 * d]] + high[req_ref[2 * d + 1]]
        return carry

    lax.fori_loop(0, DEVS, put, 0, unroll=8)
    tail = pltpu.make_async_copy(
        both.at[:, pl.ds(0, 24)], out_ref.at[:, pl.ds(2 * MAIN, 24)], sems.at[1]
    )
    tail.start()
    main = out_ref.at[:, pl.ds(0, 2 * MAIN)]
    pltpu.make_async_copy(main, main, sems.at[0]).wait()
    tail.wait()


SEND_SCRATCH = [
    pltpu.VMEM((BLK, 32, VERT), BF16),
    pltpu.VMEM((BLK, 32, VERT), BF16),
    pltpu.VMEM((DEVS, 32, VERT), BF16),
    pltpu.SemaphoreType.DMA((2,)),
]


def send_kernel(req_ref, field_ref, out_ref, slab, low, high, both, sems):
    slab[...] = field_ref[:, :MAIN, :]
    for b in range(BLK):
        low[b], high[b] = ends(field_ref[b, MAIN:, :])
    send_all(req_ref, slab, low, high, both, out_ref, sems)


def pack_field(req, field):
    return pl.pallas_call(
        send_kernel,
        grid_spec=grid_spec(
            1,
            1,
            [whole(BLK, CH, VERT)],
            pl.BlockSpec(memory_space=pltpu.HBM),
            [pltpu.VMEM((BLK, MAIN, VERT), BF16), *SEND_SCRATCH],
        ),
        out_shape=pltpu.HBM((DEVS, WIRE, VERT), BF16),
        cost_estimate=cost(1e7),
        compiler_params=params(8),
        name="pack_field",
    )(req, field)


def thirds(value):
    high = value.astype(BF16).astype(F32)
    rest = value - high
    middle = rest.astype(BF16).astype(F32)
    return high, middle, (rest - middle).astype(BF16).astype(F32)


NEAR_TERMS = ((0, 0), (0, 1), (1, 0), (1, 1), (0, 2), (2, 0))
FAR_TERMS = ((0, 0), (0, 1), (0, 2))


def stack_rows(parts):
    return jnp.concatenate(parts, axis=0)


def source_rows(geo, terms):
    parts = thirds(geo) if len(terms) > 3 else (geo,)
    square = geo[0:1] * geo[0:1] + geo[1:2] * geo[1:2] + geo[2:3] * geo[2:3] + 1.0
    facing = geo[3:4] * geo[0:1] + geo[4:5] * geo[1:2] + geo[5:6] * geo[2:3]
    zero = jnp.zeros((1, VERT), F32)
    alone = stack_rows([*thirds(square), *thirds(facing), zero, zero])
    return stack_rows([*[parts[i] for i, _ in terms], alone]).T.astype(BF16)


def receiver_rows(pos, nrm, terms):
    zero = jnp.zeros((1, VERT), F32)
    zeros3 = jnp.zeros((3, VERT), F32)
    one = jnp.ones((1, VERT), F32)
    square = pos[0:1] * pos[0:1] + pos[1:2] * pos[1:2] + pos[2:3] * pos[2:3]
    facing = nrm[0:1] * pos[0:1] + nrm[1:2] * pos[1:2] + nrm[2:3] * pos[2:3]
    forms = (
        (stack_rows([-2.0 * pos, zeros3, square, zero]), (1.0, 0.0)),
        (stack_rows([nrm, zeros3, -facing, zero]), (0.0, 0.0)),
        (stack_rows([zeros3, -pos, zero, zero]), (0.0, 1.0)),
    )
    out = []
    for rows, (with_square, with_facing) in forms:
        parts = thirds(rows)
        alone = stack_rows([one * with_square] * 3 + [one * with_facing] * 3 + [zero, zero])
        out.append(stack_rows([*[parts[j] for _, j in terms], alone]))
    return jnp.concatenate(out, axis=1).astype(BF16)


def fill_tiles(index_of, count, recv, table, out_ref):
    right = recv[...]
    for j in range(count):
        got = jnp.dot(table[index_of(j)], right, preferred_element_type=F32)
        soft = got[:, :VERT]
        value = jnp.maximum(got[:, VERT : 2 * VERT], 0.0) * jnp.maximum(got[:, 2 * VERT :], 0.0)
        value = value / (soft * soft)
        out_ref[0, j * VERT : (j + 1) * VERT, :] = value.astype(BF16)


def product(left, right):
    return jnp.dot(left, right, preferred_element_type=F32)


def near_kernel(idx_ref, field_ref, pos_ref, nrm_ref, area_ref, tiles_ref, sum_ref, table, recv, rows):
    s = pl.program_id(0)

    @pl.when(s == 0)
    def _():
        def make(t, carry):
            scaled = nrm_ref[t] * (area_ref[t] * (-1.0 / math.pi))
            geo = stack_rows([pos_ref[t], scaled, jnp.ones((2, VERT), F32)])
            table[t] = source_rows(geo, NEAR_TERMS)
            return carry

        lax.fori_loop(0, BLK, make, 0)

    recv[...] = receiver_rows(pos_ref[s], nrm_ref[s], NEAR_TERMS)
    fill_tiles(lambda j: idx_ref[s * PAIRS + j], NEAR, recv, table, tiles_ref)
    for j in range(NEAR):
        rows[:, j * VERT : (j + 1) * VERT] = field_ref[idx_ref[s * PAIRS + j]]
    sum_ref[0] = product(rows[...], tiles_ref[0])


NEAR_K = 8 * (len(NEAR_TERMS) + 1)
FAR_K = 8 * (len(FAR_TERMS) + 1)


def near_first(idx, field, pos, nrm, area):
    return pl.pallas_call(
        near_kernel,
        grid_spec=grid_spec(
            1,
            BLK,
            [whole(BLK, CH, VERT), whole(BLK, 3, VERT), whole(BLK, 3, VERT), whole(BLK, 1, VERT)],
            [slot(NEAR * VERT, VERT), slot(CH, VERT)],
            [
                pltpu.VMEM((BLK, VERT, NEAR_K), BF16),
                pltpu.VMEM((NEAR_K, 3 * VERT), BF16),
                pltpu.VMEM((CH, NEAR * VERT), BF16),
            ],
        ),
        out_shape=(
            pltpu.HBM((BLK, NEAR * VERT, VERT), BF16),
            jax.ShapeDtypeStruct((BLK, CH, VERT), F32),
        ),
        cost_estimate=cost(6e8),
        compiler_params=params(),
        name="near_first",
    )(idx, field, pos, nrm, area)


def near_again_kernel(idx_ref, field_ref, tiles_ref, sum_ref, rows, tiles, sems):
    s = pl.program_id(0)

    def copies(at):
        return pltpu.make_async_copy(tiles_ref.at[at], tiles.at[at], sems.at[at])

    @pl.when(s == 0)
    def _():
        for at in range(BLK):
            copies(at).start()

    copies(s).wait()
    for j in range(NEAR):
        rows[:, j * VERT : (j + 1) * VERT] = field_ref[idx_ref[s * PAIRS + j]]
    sum_ref[0] = product(rows[...], tiles[s])


def near_again(idx, field, tiles):
    return pl.pallas_call(
        near_again_kernel,
        grid_spec=grid_spec(
            1,
            BLK,
            [whole(BLK, CH, VERT), pl.BlockSpec(memory_space=pltpu.HBM)],
            slot(CH, VERT),
            [
                pltpu.VMEM((CH, NEAR * VERT), BF16),
                pltpu.VMEM((BLK, NEAR * VERT, VERT), BF16),
                pltpu.SemaphoreType.DMA((BLK,)),
            ],
        ),
        out_shape=jax.ShapeDtypeStruct((BLK, CH, VERT), F32),
        cost_estimate=cost(3e8),
        compiler_params=params(),
        name="near_again",
    )(idx, field, in_hbm(tiles))


def far_tiles_kernel(idx_ref, got_ref, pos_ref, nrm_ref, tiles_ref, table, recv):
    s = pl.program_id(0)

    @pl.when(s == 0)
    def _():
        def make(d, carry):
            got = [got_ref[d, i].astype(F32) for i in range(3)]
            ones = jnp.ones((2, VERT), F32)
            for k in range(CAP):
                parts = [g[2 * k : 2 * k + 1] for g in got] + [g[2 * k + 1 : 2 * k + 2] for g in got]
                table[CAP * d + k] = source_rows(stack_rows([*parts, ones]), FAR_TERMS)
            return carry

        lax.fori_loop(0, DEVS, make, 0, unroll=2)

    recv[...] = receiver_rows(pos_ref[s], nrm_ref[s], FAR_TERMS)
    fill_tiles(lambda j: idx_ref[s * PAIRS + NEAR + j], FAR, recv, table, tiles_ref)


def far_tiles(idx, got, pos, nrm):
    return pl.pallas_call(
        far_tiles_kernel,
        grid_spec=grid_spec(
            1,
            BLK,
            [whole(DEVS, 3, 4, VERT), whole(BLK, 3, VERT), whole(BLK, 3, VERT)],
            slot(FAR * VERT, VERT),
            [pltpu.VMEM((ROWS, VERT, FAR_K), BF16), pltpu.VMEM((FAR_K, 3 * VERT), BF16)],
        ),
        out_shape=pltpu.HBM((BLK, FAR * VERT, VERT), BF16),
        cost_estimate=cost(6e8),
        compiler_params=params(),
        name="far_tiles",
    )(idx, got, pos, nrm)


def far_kernel(
    idx_any,
    req_any,
    got_ref,
    tiles_ref,
    near_ref,
    albedo_ref,
    area_ref,
    share_ref,
    out_ref,
    energy_ref,
    *more,
    send,
):
    if send:
        wire_ref, idx_ref, req_ref, rows, field, last, tiles, sems, slab, low, high, both, out_sems = more
    else:
        idx_ref, req_ref, rows, field, last, tiles, sems = more
    ahead = 5
    arrived = pltpu.make_async_copy(got_ref, field.at[:, pl.ds(0, WIRE)], sems.at[BLK])
    arrived.start()

    def copies(at):
        return pltpu.make_async_copy(tiles_ref.at[at], tiles.at[at], sems.at[at])

    small = [pltpu.make_async_copy(idx_any, idx_ref, sems.at[BLK + 1])]
    if send:
        small.append(pltpu.make_async_copy(req_any, req_ref, sems.at[BLK + 2]))
    for one in small:
        one.start()
    for at in range(ahead):
        copies(at).start()
    for one in small:
        one.wait()
    arrived.wait()
    for at in range(ahead, BLK):
        copies(at).start()

    def split(d, carry):
        both_ends = field[d, 2 * MAIN : 2 * MAIN + 32]
        last[2 * d] = both_ends[0:16]
        last[2 * d + 1] = both_ends[SECOND : SECOND + 16]
        return carry

    lax.fori_loop(0, DEVS, split, 0, unroll=8)
    channel = lax.broadcasted_iota(I32, (CH, VERT), 0)

    def gather(s, rows):
        for j in range(FAR):
            row = idx_ref[s * PAIRS + NEAR + j]
            cols = slice(j * VERT, (j + 1) * VERT)
            at = pl.multiple_of((row & 1) * MAIN, MAIN)
            rows[0:MAIN, cols] = field[row >> 1, pl.ds(at, MAIN)]
            rows[MAIN : MAIN + 16, cols] = last[row]

    def finish(s, got):
        total = near_ref[s] + got[:CH]
        shade = jnp.where(
            channel < CH // COLORS,
            albedo_ref[s, 0:1, :],
            jnp.where(channel < 2 * (CH // COLORS), albedo_ref[s, 1:2, :], albedo_ref[s, 2:3, :]),
        )
        bounce = total * shade
        rounded = bounce.astype(BF16)
        out_ref[s] = rounded
        if send:
            slab[s] = rounded[:MAIN]
            low[s], high[s] = ends(rounded[MAIN:])
        return jnp.sum(area_ref[s] * bounce * bounce, axis=0, keepdims=True)

    def group(h, energy):
        these = [h * GROUP + i for i in range(GROUP)]
        for s in these:
            copies(s).wait()
        for i, s in enumerate(these):
            gather(s, rows.at[i])
        results = [product(rows[i], tiles[s]) for i, s in enumerate(these)]
        for s, got in zip(these, results):
            energy = energy + finish(s, got)
        return energy

    energy = lax.fori_loop(0, BLK // GROUP, group, jnp.zeros((1, VERT), F32)) * INV_COUNT
    if send:
        energy_ref[...] = energy
        send_all(req_ref, slab, low, high, both, wire_ref, out_sems)
    else:
        shares = jnp.concatenate([share_ref[...], energy], axis=0)
        energy_ref[...] = jnp.broadcast_to(shares[None], (DEVS, 2, VERT))


GROUP = 2
INV_COUNT = 1.0 / (DEVS * BLK * VERT * CH)


def far_bounce(idx, req, got, tiles, near, albedo, area, share, send):
    hbm = pl.BlockSpec(memory_space=pltpu.HBM)
    vmem = pl.BlockSpec(memory_space=pltpu.VMEM)
    any_space = pl.BlockSpec(memory_space=pl.ANY)
    return pl.pallas_call(
        functools.partial(far_kernel, send=send),
        grid_spec=grid_spec(
            0,
            1,
            [any_space, any_space, hbm, hbm, vmem, vmem, vmem, vmem],
            [vmem, vmem] + [hbm] * send,
            [
                pltpu.SMEM((BLK * PAIRS,), I32),
                pltpu.SMEM((ROWS,), I32),
                pltpu.VMEM((GROUP, MAIN + 16, FAR * VERT), BF16),
                pltpu.VMEM((DEVS, WIRE + 8, VERT), BF16),
                pltpu.VMEM((ROWS, 16, VERT), BF16),
                pltpu.VMEM((BLK, FAR * VERT, VERT), BF16),
                pltpu.SemaphoreType.DMA((BLK + 3,)),
            ]
            + [pltpu.VMEM((BLK, MAIN, VERT), BF16), *SEND_SCRATCH] * send,
        ),
        out_shape=[
            jax.ShapeDtypeStruct((BLK, CH, VERT), BF16),
            jax.ShapeDtypeStruct((1, VERT) if send else (DEVS, 2, VERT), F32),
        ]
        + [pltpu.HBM((DEVS, WIRE, VERT), BF16)] * send,
        cost_estimate=cost(5e8),
        compiler_params=params(),
        name="far_bounce_one" if send else "far_bounce_two",
    )(idx, req, in_hbm(got), in_hbm(tiles), near, albedo, area, share)


def swap(value):
    return lax.all_to_all(value, AXES, split_axis=0, concat_axis=0, tiled=True)


def body(transfer, positions, normals, area, albedo, pairs, home):
    area_row = area.reshape(BLK, 1, VERT)
    home = home.reshape(BLK, VERT)
    need = find_requests(pairs, home)
    idx = find_indices(pairs, home, need).reshape(-1)
    sources = source_table(positions, normals, area_row)
    asked = swap(need.reshape(DEVS, 1, CAP))
    geometry = swap(pack_geometry(asked, sources))
    asked = asked.reshape(-1)
    got_one = swap(pack_field(asked, transfer))
    near_tiles, near_one = near_first(idx, transfer, positions, normals, area_row)
    tiles = far_tiles(idx, geometry, positions, normals)
    none = jnp.zeros((1, VERT), F32)
    bounce_one, share_one, wire = far_bounce(
        idx, asked, got_one, tiles, near_one, albedo, area_row, none, True
    )
    got_two = swap(wire)
    near_two = near_again(idx, bounce_one, near_tiles)
    bounce_two, shares = far_bounce(
        idx, asked, got_two, tiles, near_two, albedo, area_row, share_one, False
    )
    energies = jnp.sum(swap(shares), axis=(0, 2))
    return bounce_one, bounce_two, energies


def solution(mesh):
    finer = Mesh(mesh.devices.reshape(4, 2, 4, 4), AXES)
    three = P(AXES, None, None)
    return jax.shard_map(
        body,
        mesh=finer,
        in_specs=(three, three, three, P(AXES, None), three, P(AXES, None), P()),
        out_specs=(three, three, P()),
        check_vma=False,
    )
```

```python
import functools
import math

import jax
import jax.numpy as jnp
from jax import lax
from jax.experimental import pallas as pl
from jax.experimental.pallas import tpu as pltpu
from jax.sharding import Mesh
from jax.sharding import PartitionSpec as P

COLORS = 3
NEAR = 16
FAR = 24
PAIRS = NEAR + FAR
CAP = 2
CH = 75
MAIN = 64
REST = CH - MAIN
SECOND = 12
WIRE = 2 * MAIN + 24
BLK = 16
VERT = 128
DEVS = 128
ROWS = DEVS * CAP
AXES = ("gx_0", "gx_1", "gy_0", "gy_1")

F32 = jnp.float32
BF16 = jnp.bfloat16
I32 = jnp.int32


def in_hbm(value):
    return pltpu.with_memory_space_constraint(value, pltpu.HBM)


def params(limit_mib=40):
    return pltpu.CompilerParams(
        dimension_semantics=("arbitrary",), vmem_limit_bytes=limit_mib * 1024 * 1024
    )


def cost(flops, read=0):
    return pl.CostEstimate(flops=int(flops), bytes_accessed=int(read), transcendentals=0)


TOGETHER = 4


def home_parts(home):
    return jnp.concatenate([home >> 4, home & 15], axis=0).astype(F32).astype(BF16)


def look_up(both, blocks):
    wide = blocks.shape[1]
    sub = lax.broadcasted_iota(I32, (VERT, wide), 0)
    hot = jnp.where(sub == (blocks & 127), 1.0, 0.0).astype(BF16)
    got = jnp.dot(both, hot, preferred_element_type=F32)
    here = lax.broadcasted_iota(I32, (16, wide), 0) == (blocks >> 7)
    owner = jnp.sum(jnp.where(here, got[:16], 0.0), axis=0, keepdims=True)
    local = jnp.sum(jnp.where(here, got[16:], 0.0), axis=0, keepdims=True)
    return owner, local


def request_kernel(pairs_hbm, home_hbm, req_ref, pairs_ref, home_ref, sems):
    first = pltpu.make_async_copy(pairs_hbm, pairs_ref, sems.at[0])
    second = pltpu.make_async_copy(home_hbm, home_ref, sems.at[1])
    first.start()
    second.start()
    first.wait()
    second.wait()
    both = home_parts(home_ref[...])
    far = pairs_ref[...][:, NEAR:]
    wide = TOGETHER * FAR
    device = lax.broadcasted_iota(I32, (VERT, wide), 0).astype(F32)
    least = jnp.full((VERT, wide), 99.0, F32)
    most = jnp.full((VERT, wide), -1.0, F32)
    for g in range(BLK // TOGETHER):
        rows = [far[g * TOGETHER + i : g * TOGETHER + i + 1] for i in range(TOGETHER)]
        owner, local = look_up(both, jnp.concatenate(rows, axis=1))
        same = device == owner
        least = jnp.minimum(least, jnp.where(same, local, 99.0))
        most = jnp.maximum(most, jnp.where(same, local, -1.0))
    lo = jnp.min(least, axis=1, keepdims=True)
    hi = jnp.max(most, axis=1, keepdims=True)
    used = hi >= 0.0
    req_ref[:, 0:1] = jnp.where(used, lo, 0.0).astype(I32)
    req_ref[:, 1:2] = jnp.where(used, hi, 0.0).astype(I32)


def find_requests(pairs, home):
    return pl.pallas_call(
        request_kernel,
        out_shape=jax.ShapeDtypeStruct((DEVS, CAP), I32),
        in_specs=[pl.BlockSpec(memory_space=pltpu.HBM), pl.BlockSpec(memory_space=pltpu.HBM)],
        scratch_shapes=[
            pltpu.VMEM((BLK, PAIRS), I32),
            pltpu.VMEM((BLK, VERT), I32),
            pltpu.SemaphoreType.DMA((2,)),
        ],
        cost_estimate=cost(2e6),
        compiler_params=pltpu.CompilerParams(vmem_limit_bytes=8 * 1024 * 1024),
        name="requests",
    )(in_hbm(pairs), in_hbm(home))


def index_kernel(pairs_ref, home_ref, req_ref, idx_ref):
    both = home_parts(home_ref[...])
    pairs = pairs_ref[...]
    device = lax.broadcasted_iota(I32, (VERT, PAIRS), 0).astype(F32)
    lane = lax.broadcasted_iota(I32, (1, PAIRS), 1)
    lo = req_ref[:, 0:1].astype(F32)
    for s in range(BLK):
        owner, local = look_up(both, pairs[s : s + 1, :])
        first = jnp.sum(jnp.where(device == owner, lo, 0.0), axis=0, keepdims=True)
        far_row = owner * 2.0 + jnp.where(local == first, 0.0, 1.0)
        idx_ref[s : s + 1, :] = jnp.where(lane < NEAR, local, far_row).astype(I32)


def find_indices(pairs, home, need):
    return pl.pallas_call(
        index_kernel,
        out_shape=jax.ShapeDtypeStruct((BLK, PAIRS), I32),
        cost_estimate=cost(4e6),
        compiler_params=pltpu.CompilerParams(vmem_limit_bytes=8 * 1024 * 1024),
        name="indices",
    )(pairs, home, need)


def whole(*shape):
    return pl.BlockSpec(shape, lambda i, *_: (0,) * len(shape))


def slot(*shape):
    return pl.BlockSpec((1,) + shape, lambda i, *_: (i,) + (0,) * len(shape))


def grid_spec(prefetch, steps, in_specs, out_specs, scratch):
    return pltpu.PrefetchScalarGridSpec(
        num_scalar_prefetch=prefetch,
        grid=(steps,),
        in_specs=in_specs,
        out_specs=out_specs,
        scratch_shapes=scratch,
    )


def table_kernel(pos_ref, nrm_ref, area_ref, out_ref):
    scaled = nrm_ref[...] * (area_ref[...] * (-1.0 / math.pi))
    for i in range(3):
        both = jnp.concatenate([pos_ref[:, i : i + 1, :], scaled[:, i : i + 1, :]], axis=1)
        out_ref[:, i] = both.astype(BF16)


def source_table(pos, nrm, area):
    return pl.pallas_call(
        table_kernel,
        out_shape=jax.ShapeDtypeStruct((BLK, 3, 2, VERT), BF16),
        cost_estimate=cost(1e6),
        compiler_params=pltpu.CompilerParams(vmem_limit_bytes=8 * 1024 * 1024),
        name="source_table",
    )(pos, nrm, area)


def geometry_kernel(asked_ref, table, out_ref, across, req_ref, sem):
    asked = asked_ref[:, 0, :].astype(F32).astype(BF16)
    row = lax.broadcasted_iota(I32, (DEVS, DEVS), 0)
    same = jnp.where(row == lax.broadcasted_iota(I32, (DEVS, DEVS), 1), 1.0, 0.0).astype(BF16)
    turned = lax.dot_general(asked, same, (((0,), (0,)), ((), ())), preferred_element_type=F32)
    across[...] = turned.astype(I32)
    copy = pltpu.make_async_copy(across, req_ref, sem)
    copy.start()
    copy.wait()

    def put(d, carry):
        for k in range(CAP):
            out_ref[d, :, 2 * k : 2 * k + 2, :] = table[req_ref[k, d]]
        return carry

    lax.fori_loop(0, DEVS, put, 0, unroll=8)


def pack_geometry(asked, table):
    return pl.pallas_call(
        geometry_kernel,
        out_shape=jax.ShapeDtypeStruct((DEVS, 3, 4, VERT), BF16),
        scratch_shapes=[
            pltpu.VMEM((CAP, DEVS), I32),
            pltpu.SMEM((CAP, DEVS), I32),
            pltpu.SemaphoreType.DMA,
        ],
        cost_estimate=cost(2e6),
        compiler_params=pltpu.CompilerParams(vmem_limit_bytes=8 * 1024 * 1024),
        name="pack_geometry",
    )(asked, table)


def ends(last):
    last = last.astype(F32)
    zeros = lambda n: jnp.zeros((n, VERT), F32)
    low = jnp.concatenate([last, zeros(32 - REST)], axis=0)
    high = jnp.concatenate([zeros(SECOND), last, zeros(32 - SECOND - REST)], axis=0)
    return low.astype(BF16), high.astype(BF16)


def send_all(req_ref, slab, low, high, both, out_ref, sems):
    def main_rows(d, carry):
        for k in range(CAP):
            pltpu.make_async_copy(
                slab.at[req_ref[2 * d + k]], out_ref.at[d, pl.ds(k * MAIN, MAIN)], sems.at[0]
            ).start()
        return carry

    lax.fori_loop(0, DEVS, main_rows, 0, unroll=16)

    def put(d, carry):
        both[d] = low[req_ref[2 * d]] + high[req_ref[2 * d + 1]]
        return carry

    lax.fori_loop(0, DEVS, put, 0, unroll=8)
    tail = pltpu.make_async_copy(
        both.at[:, pl.ds(0, 24)], out_ref.at[:, pl.ds(2 * MAIN, 24)], sems.at[1]
    )
    tail.start()
    main = out_ref.at[:, pl.ds(0, 2 * MAIN)]
    pltpu.make_async_copy(main, main, sems.at[0]).wait()
    tail.wait()


SEND_SCRATCH = [
    pltpu.VMEM((BLK, 32, VERT), BF16),
    pltpu.VMEM((BLK, 32, VERT), BF16),
    pltpu.VMEM((DEVS, 32, VERT), BF16),
    pltpu.SemaphoreType.DMA((2,)),
]


def send_kernel(req_ref, field_ref, out_ref, slab, low, high, both, sems):
    slab[...] = field_ref[:, :MAIN, :]
    for b in range(BLK):
        low[b], high[b] = ends(field_ref[b, MAIN:, :])
    send_all(req_ref, slab, low, high, both, out_ref, sems)


def pack_field(req, field):
    return pl.pallas_call(
        send_kernel,
        grid_spec=grid_spec(
            1,
            1,
            [whole(BLK, CH, VERT)],
            pl.BlockSpec(memory_space=pltpu.HBM),
            [pltpu.VMEM((BLK, MAIN, VERT), BF16), *SEND_SCRATCH],
        ),
        out_shape=pltpu.HBM((DEVS, WIRE, VERT), BF16),
        cost_estimate=cost(1e7),
        compiler_params=params(8),
        name="pack_field",
    )(req, field)


def thirds(value):
    high = value.astype(BF16).astype(F32)
    rest = value - high
    middle = rest.astype(BF16).astype(F32)
    return high, middle, (rest - middle).astype(BF16).astype(F32)


NEAR_TERMS = ((0, 0), (0, 1), (1, 0), (1, 1), (0, 2), (2, 0))
FAR_TERMS = ((0, 0), (0, 1), (0, 2))


def stack_rows(parts):
    return jnp.concatenate(parts, axis=0)


def source_rows(geo, terms):
    parts = thirds(geo) if len(terms) > 3 else (geo,)
    square = geo[0:1] * geo[0:1] + geo[1:2] * geo[1:2] + geo[2:3] * geo[2:3] + 1.0
    facing = geo[3:4] * geo[0:1] + geo[4:5] * geo[1:2] + geo[5:6] * geo[2:3]
    zero = jnp.zeros((1, VERT), F32)
    alone = stack_rows([*thirds(square), *thirds(facing), zero, zero])
    return stack_rows([*[parts[i] for i, _ in terms], alone]).T.astype(BF16)


def receiver_rows(pos, nrm, terms):
    zero = jnp.zeros((1, VERT), F32)
    zeros3 = jnp.zeros((3, VERT), F32)
    one = jnp.ones((1, VERT), F32)
    square = pos[0:1] * pos[0:1] + pos[1:2] * pos[1:2] + pos[2:3] * pos[2:3]
    facing = nrm[0:1] * pos[0:1] + nrm[1:2] * pos[1:2] + nrm[2:3] * pos[2:3]
    forms = (
        (stack_rows([-2.0 * pos, zeros3, square, zero]), (1.0, 0.0)),
        (stack_rows([nrm, zeros3, -facing, zero]), (0.0, 0.0)),
        (stack_rows([zeros3, -pos, zero, zero]), (0.0, 1.0)),
    )
    out = []
    for rows, (with_square, with_facing) in forms:
        parts = thirds(rows)
        alone = stack_rows([one * with_square] * 3 + [one * with_facing] * 3 + [zero, zero])
        out.append(stack_rows([*[parts[j] for _, j in terms], alone]))
    return jnp.concatenate(out, axis=1).astype(BF16)


def fill_tiles(index_of, count, recv, table, out_ref):
    right = recv[...]
    for j in range(count):
        got = jnp.dot(table[index_of(j)], right, preferred_element_type=F32)
        soft = got[:, :VERT]
        value = jnp.maximum(got[:, VERT : 2 * VERT], 0.0) * jnp.maximum(got[:, 2 * VERT :], 0.0)
        value = value / (soft * soft)
        out_ref[0, j * VERT : (j + 1) * VERT, :] = value.astype(BF16)


def product(left, right):
    return jnp.dot(left, right, preferred_element_type=F32)


def near_kernel(idx_ref, field_ref, pos_ref, nrm_ref, area_ref, tiles_ref, sum_ref, table, recv, rows):
    s = pl.program_id(0)

    @pl.when(s == 0)
    def _():
        def make(t, carry):
            scaled = nrm_ref[t] * (area_ref[t] * (-1.0 / math.pi))
            geo = stack_rows([pos_ref[t], scaled, jnp.ones((2, VERT), F32)])
            table[t] = source_rows(geo, NEAR_TERMS)
            return carry

        lax.fori_loop(0, BLK, make, 0)

    recv[...] = receiver_rows(pos_ref[s], nrm_ref[s], NEAR_TERMS)
    fill_tiles(lambda j: idx_ref[s * PAIRS + j], NEAR, recv, table, tiles_ref)
    for j in range(NEAR):
        rows[:, j * VERT : (j + 1) * VERT] = field_ref[idx_ref[s * PAIRS + j]]
    sum_ref[0] = product(rows[...], tiles_ref[0])


NEAR_K = 8 * (len(NEAR_TERMS) + 1)
FAR_K = 8 * (len(FAR_TERMS) + 1)


def near_first(idx, field, pos, nrm, area):
    return pl.pallas_call(
        near_kernel,
        grid_spec=grid_spec(
            1,
            BLK,
            [whole(BLK, CH, VERT), whole(BLK, 3, VERT), whole(BLK, 3, VERT), whole(BLK, 1, VERT)],
            [slot(NEAR * VERT, VERT), slot(CH, VERT)],
            [
                pltpu.VMEM((BLK, VERT, NEAR_K), BF16),
                pltpu.VMEM((NEAR_K, 3 * VERT), BF16),
                pltpu.VMEM((CH, NEAR * VERT), BF16),
            ],
        ),
        out_shape=(
            pltpu.HBM((BLK, NEAR * VERT, VERT), BF16),
            jax.ShapeDtypeStruct((BLK, CH, VERT), F32),
        ),
        cost_estimate=cost(6e8),
        compiler_params=params(),
        name="near_first",
    )(idx, field, pos, nrm, area)


def near_again_kernel(idx_ref, field_ref, tiles_ref, sum_ref, rows, tiles, sems):
    s = pl.program_id(0)

    def copies(at):
        return pltpu.make_async_copy(tiles_ref.at[at], tiles.at[at], sems.at[at])

    @pl.when(s == 0)
    def _():
        for at in range(BLK):
            copies(at).start()

    copies(s).wait()
    for j in range(NEAR):
        rows[:, j * VERT : (j + 1) * VERT] = field_ref[idx_ref[s * PAIRS + j]]
    sum_ref[0] = product(rows[...], tiles[s])


def near_again(idx, field, tiles):
    return pl.pallas_call(
        near_again_kernel,
        grid_spec=grid_spec(
            1,
            BLK,
            [whole(BLK, CH, VERT), pl.BlockSpec(memory_space=pltpu.HBM)],
            slot(CH, VERT),
            [
                pltpu.VMEM((CH, NEAR * VERT), BF16),
                pltpu.VMEM((BLK, NEAR * VERT, VERT), BF16),
                pltpu.SemaphoreType.DMA((BLK,)),
            ],
        ),
        out_shape=jax.ShapeDtypeStruct((BLK, CH, VERT), F32),
        cost_estimate=cost(3e8),
        compiler_params=params(),
        name="near_again",
    )(idx, field, in_hbm(tiles))


def far_tiles_kernel(idx_ref, got_ref, pos_ref, nrm_ref, tiles_ref, table, recv):
    s = pl.program_id(0)

    @pl.when(s == 0)
    def _():
        def make(d, carry):
            got = [got_ref[d, i].astype(F32) for i in range(3)]
            ones = jnp.ones((2, VERT), F32)
            for k in range(CAP):
                parts = [g[2 * k : 2 * k + 1] for g in got] + [g[2 * k + 1 : 2 * k + 2] for g in got]
                table[CAP * d + k] = source_rows(stack_rows([*parts, ones]), FAR_TERMS)
            return carry

        lax.fori_loop(0, DEVS, make, 0, unroll=2)

    recv[...] = receiver_rows(pos_ref[s], nrm_ref[s], FAR_TERMS)
    fill_tiles(lambda j: idx_ref[s * PAIRS + NEAR + j], FAR, recv, table, tiles_ref)


def far_tiles(idx, got, pos, nrm):
    return pl.pallas_call(
        far_tiles_kernel,
        grid_spec=grid_spec(
            1,
            BLK,
            [whole(DEVS, 3, 4, VERT), whole(BLK, 3, VERT), whole(BLK, 3, VERT)],
            slot(FAR * VERT, VERT),
            [pltpu.VMEM((ROWS, VERT, FAR_K), BF16), pltpu.VMEM((FAR_K, 3 * VERT), BF16)],
        ),
        out_shape=pltpu.HBM((BLK, FAR * VERT, VERT), BF16),
        cost_estimate=cost(6e8),
        compiler_params=params(),
        name="far_tiles",
    )(idx, got, pos, nrm)


def far_kernel(
    idx_any,
    req_any,
    got_ref,
    tiles_ref,
    near_ref,
    albedo_ref,
    area_ref,
    share_ref,
    out_ref,
    energy_ref,
    *more,
    send,
):
    if send:
        wire_ref, idx_ref, req_ref, rows, field, last, tiles, sems, slab, low, high, both, out_sems = more
    else:
        idx_ref, req_ref, rows, field, last, tiles, sems = more
    ahead = 5
    arrived = pltpu.make_async_copy(got_ref, field.at[:, pl.ds(0, WIRE)], sems.at[BLK])
    arrived.start()

    def copies(at):
        return pltpu.make_async_copy(tiles_ref.at[at], tiles.at[at], sems.at[at])

    small = [pltpu.make_async_copy(idx_any, idx_ref, sems.at[BLK + 1])]
    if send:
        small.append(pltpu.make_async_copy(req_any, req_ref, sems.at[BLK + 2]))
    for one in small:
        one.start()
    for at in range(ahead):
        copies(at).start()
    for one in small:
        one.wait()
    arrived.wait()
    for at in range(ahead, BLK):
        copies(at).start()

    def split(d, carry):
        both_ends = field[d, 2 * MAIN : 2 * MAIN + 32]
        last[2 * d] = both_ends[0:16]
        last[2 * d + 1] = both_ends[SECOND : SECOND + 16]
        return carry

    lax.fori_loop(0, DEVS, split, 0, unroll=8)
    channel = lax.broadcasted_iota(I32, (CH, VERT), 0)

    def gather(s, rows):
        for j in range(FAR):
            row = idx_ref[s * PAIRS + NEAR + j]
            cols = slice(j * VERT, (j + 1) * VERT)
            at = pl.multiple_of((row & 1) * MAIN, MAIN)
            rows[0:MAIN, cols] = field[row >> 1, pl.ds(at, MAIN)]
            rows[MAIN : MAIN + 16, cols] = last[row]

    def finish(s, got):
        total = near_ref[s] + got[:CH]
        shade = jnp.where(
            channel < CH // COLORS,
            albedo_ref[s, 0:1, :],
            jnp.where(channel < 2 * (CH // COLORS), albedo_ref[s, 1:2, :], albedo_ref[s, 2:3, :]),
        )
        bounce = total * shade
        rounded = bounce.astype(BF16)
        out_ref[s] = rounded
        if send:
            slab[s] = rounded[:MAIN]
            low[s], high[s] = ends(rounded[MAIN:])
        return jnp.sum(area_ref[s] * bounce * bounce, axis=0, keepdims=True)

    def group(h, energy):
        these = [h * GROUP + i for i in range(GROUP)]
        for s in these:
            copies(s).wait()
        for i, s in enumerate(these):
            gather(s, rows.at[i])
        results = [product(rows[i], tiles[s]) for i, s in enumerate(these)]
        for s, got in zip(these, results):
            energy = energy + finish(s, got)
        return energy

    energy = lax.fori_loop(0, BLK // GROUP, group, jnp.zeros((1, VERT), F32)) * INV_COUNT
    if send:
        energy_ref[...] = energy
        send_all(req_ref, slab, low, high, both, wire_ref, out_sems)
    else:
        shares = jnp.concatenate([share_ref[...], energy], axis=0)
        energy_ref[...] = jnp.broadcast_to(shares[None], (DEVS, 2, VERT))


GROUP = 2
INV_COUNT = 1.0 / (DEVS * BLK * VERT * CH)


def far_bounce(idx, req, got, tiles, near, albedo, area, share, send):
    hbm = pl.BlockSpec(memory_space=pltpu.HBM)
    vmem = pl.BlockSpec(memory_space=pltpu.VMEM)
    any_space = pl.BlockSpec(memory_space=pl.ANY)
    return pl.pallas_call(
        functools.partial(far_kernel, send=send),
        grid_spec=grid_spec(
            0,
            1,
            [any_space, any_space, hbm, hbm, vmem, vmem, vmem, vmem],
            [vmem, vmem] + [hbm] * send,
            [
                pltpu.SMEM((BLK * PAIRS,), I32),
                pltpu.SMEM((ROWS,), I32),
                pltpu.VMEM((GROUP, MAIN + 16, FAR * VERT), BF16),
                pltpu.VMEM((DEVS, WIRE + 8, VERT), BF16),
                pltpu.VMEM((ROWS, 16, VERT), BF16),
                pltpu.VMEM((BLK, FAR * VERT, VERT), BF16),
                pltpu.SemaphoreType.DMA((BLK + 3,)),
            ]
            + [pltpu.VMEM((BLK, MAIN, VERT), BF16), *SEND_SCRATCH] * send,
        ),
        out_shape=[
            jax.ShapeDtypeStruct((BLK, CH, VERT), BF16),
            jax.ShapeDtypeStruct((1, VERT) if send else (DEVS, 2, VERT), F32),
        ]
        + [pltpu.HBM((DEVS, WIRE, VERT), BF16)] * send,
        cost_estimate=cost(5e8),
        compiler_params=params(),
        name="far_bounce_one" if send else "far_bounce_two",
    )(idx, req, in_hbm(got), in_hbm(tiles), near, albedo, area, share)


def swap(value):
    return lax.all_to_all(value, AXES, split_axis=0, concat_axis=0, tiled=True)


def body(transfer, positions, normals, area, albedo, pairs, home):
    area_row = area.reshape(BLK, 1, VERT)
    home = home.reshape(BLK, VERT)
    need = find_requests(pairs, home)
    idx = find_indices(pairs, home, need).reshape(-1)
    sources = source_table(positions, normals, area_row)
    asked = swap(need.reshape(DEVS, 1, CAP))
    geometry = swap(pack_geometry(asked, sources))
    asked = asked.reshape(-1)
    got_one = swap(pack_field(asked, transfer))
    near_tiles, near_one = near_first(idx, transfer, positions, normals, area_row)
    tiles = far_tiles(idx, geometry, positions, normals)
    none = jnp.zeros((1, VERT), F32)
    bounce_one, share_one, wire = far_bounce(
        idx, asked, got_one, tiles, near_one, albedo, area_row, none, True
    )
    got_two = swap(wire)
    near_two = near_again(idx, bounce_one, near_tiles)
    bounce_two, shares = far_bounce(
        idx, asked, got_two, tiles, near_two, albedo, area_row, share_one, False
    )
    energies = jnp.sum(swap(shares), axis=(0, 2))
    return bounce_one, bounce_two, energies


def solution(mesh):
    finer = Mesh(mesh.devices.reshape(4, 2, 4, 4), AXES)
    three = P(AXES, None, None)
    return jax.shard_map(
        body,
        mesh=finer,
        in_specs=(three, three, three, P(AXES, None), three, P(AXES, None), P()),
        out_specs=(three, three, P()),
        check_vma=False,
    )
```
